32 devices in a mesh: dp: 8 (over z, core), height: 4 (over y, x).
Axes of the slice: x: 2, y: 2, z: 4, core: 2. Of those that a mesh axis runs over, the one named last changes fastest.
Arguments:
- latents: bfloat16 [8, 16, 128, 640], P('dp', 'height'), parts along dimension 0, may hold values from -20 to 20
- latent_tangent: bfloat16 [8, 16, 128, 640], P('dp', 'height'), parts along dimension 0, may hold values from -20 to 20
- gain_first: float32 [640], replicated, may hold values from 0.5 to 2
- weight_first: bfloat16 [9, 640, 640], P(None, None, 'height'), may hold values from -0.078125 to 0.078125
- gain_second: float32 [640], replicated, may hold values from 0.5 to 2
- weight_second: bfloat16 [9, 640, 640], P(None, None, 'height'), may hold values from -0.078125 to 0.078125
Outputs:
- block_output: bfloat16 [8, 16, 128, 640], P('dp', 'height'), parts along dimension 0
- output_tangent: bfloat16 [8, 16, 128, 640], P('dp', 'height'), parts along dimension 0
The draws below stay inside these ranges and needn't reach their ends.
There are 8 independent parts, one for each index of `dp`. The reference program is written for one: setup_inputs(seed, part) draws one part's arguments, and reference() takes and returns one part's arrays. A program takes and returns all parts, laid end to end along the dimension named above; an argument that names none is the same for every part. Nothing has to cross between parts.
All inputs are finite; a program needn't handle non-finite values.
Results may differ from the reference program's by a relative error of at most 0.006.
Values may be sent and summed in bfloat16 or wider, within the bound.
No kernel may reach another device: no remote copies, remote signals or barrier semaphores. Data moves between devices by JAX's collectives and lax.ppermute only.
A program may use at most 128 MiB of HBM per device.

```python
import math
import jax
import jax.numpy as jnp
from jax import lax

C = 640
GROUPS = 32
WIDTH = 128
H = 16


def rising_field(key, salt):
    folded = jax.random.fold_in(key, salt)
    first_key = jax.random.fold_in(folded, 0)
    row_frac = jnp.arange(H, dtype=jnp.float32) / max(H - 1, 1)
    row_scale = (3.0 ** row_frac)[:, None, None]
    base_values = jnp.clip(jax.random.normal(first_key, (H, WIDTH, C), jnp.float32), -6.0, 6.0)
    field = base_values * row_scale
    return jnp.clip(field, -20.0, 20.0)[None]


def draw_latents(key, part):
    return rising_field(key, 11).astype(jnp.bfloat16)


def draw_latent_tangent(key, part):
    return rising_field(key, 23).astype(jnp.bfloat16)


def block_levels(key, extent, cuts, smallest, top_value):
    def one(dim, shards_of):
        steps = jax.random.uniform(jax.random.fold_in(jax.random.fold_in(key, 6), dim), (shards_of,), jnp.float32, smallest / len(cuts), top_value / len(cuts))
        return jnp.repeat(jnp.exp(steps), extent[dim] // shards_of).reshape((-1,) + (1,) * (len(extent) - dim - 1))

    level = one(*cuts[0])
    for cut in cuts[1:]:
        level = level * one(*cut)
    return level


def noise(key, extent, spread, reach, cuts=(), kind=jnp.bfloat16):
    gain = block_levels(key, extent, cuts, -0.22, 0.18) if cuts else 1.0
    array = jax.random.normal(key, extent, jnp.float32) * spread * gain
    return jnp.minimum(jnp.maximum(array, -reach), reach).astype(kind)


def setup_inputs(seed: int = 0, part: int = 0) -> dict:
    key_list = jax.random.split(jax.random.key(seed), 7)
    part_keys = jax.random.split(jax.random.fold_in(key_list[6], part), 7)
    latents = draw_latents(jax.random.fold_in(jax.random.fold_in(key_list[6], part), 71), part)
    latent_tangent = draw_latent_tangent(jax.random.fold_in(jax.random.fold_in(key_list[6], part), 71), part)
    gain_first = jnp.clip(jnp.exp(jax.random.uniform(key_list[2], (C,), jnp.float32, math.log(0.5), math.log(2.0))), 0.5, 2.0)
    weight_first = noise(key_list[3], (9, C, C), (9 * C) ** -0.5, 0.078125, ((2, 4),))
    gain_second = jnp.clip(jnp.exp(jax.random.uniform(key_list[4], (C,), jnp.float32, math.log(0.5), math.log(2.0))), 0.5, 2.0)
    weight_second = noise(key_list[5], (9, C, C), (9 * C) ** -0.5, 0.078125, ((2, 4),))
    return {"latents": latents, "latent_tangent": latent_tangent, "gain_first": gain_first, "weight_first": weight_first, "gain_second": gain_second, "weight_second": weight_second}


epsilon = 1e-05

def normalize(primal, tangent, gain_vector):
    row_count, col_count, chans = primal.shape
    size = chans // GROUPS
    grouped = primal.reshape(row_count * col_count, GROUPS, size)
    tgrouped = tangent.reshape(row_count * col_count, GROUPS, size)
    group_mean = lax.optimization_barrier(jnp.mean(grouped, axis=(0, 2)))
    tangent_mean = lax.optimization_barrier(jnp.mean(tgrouped, axis=(0, 2)))
    centered = grouped - group_mean[None, :, None]
    tangent_centered = tgrouped - tangent_mean[None, :, None]
    variance = lax.optimization_barrier(jnp.mean(centered * centered, axis=(0, 2)))
    dvariance = 2.0 * lax.optimization_barrier(jnp.mean(centered * tangent_centered, axis=(0, 2)))
    inverse = lax.rsqrt(variance + epsilon)[None, :, None]
    normed = centered * inverse
    dnormed = tangent_centered * inverse - centered * (0.5 * dvariance[None, :, None] * inverse ** 3)
    scaled = normed.reshape(row_count, col_count, chans) * gain_vector
    dscaled = dnormed.reshape(row_count, col_count, chans) * gain_vector
    sigmoid_value = jax.nn.sigmoid(scaled)
    hidden = scaled * sigmoid_value
    dhidden = dscaled * sigmoid_value * (1.0 + scaled * (1.0 - sigmoid_value))
    return (hidden.astype(jnp.bfloat16), dhidden.astype(jnp.bfloat16))

def convolve(hidden, weight):
    row_count, col_count, chans = hidden.shape
    padded = jnp.pad(hidden, ((1, 1), (1, 1), (0, 0)))
    accumulated = jnp.zeros((row_count * col_count, weight.shape[2]), jnp.float32)
    for tap_index in range(9):
        offset_row = tap_index // 3
        offset_col = tap_index % 3
        window = padded[offset_row:offset_row + row_count, offset_col:offset_col + col_count, :].reshape(-1, chans)
        accumulated = accumulated + jnp.dot(window, weight[tap_index], preferred_element_type=jnp.float32)
    return accumulated.reshape(row_count, col_count, -1)

def reference(latents, latent_tangent, gain_first, weight_first, gain_second, weight_second):
    primal = latents[0].astype(jnp.float32)
    tangent = latent_tangent[0].astype(jnp.float32)
    hidden, dhidden = normalize(primal, tangent, gain_first)
    middle = convolve(hidden, weight_first).astype(jnp.bfloat16)
    dmiddle = convolve(dhidden, weight_first).astype(jnp.bfloat16)
    second, dsecond = normalize(middle.astype(jnp.float32), dmiddle.astype(jnp.float32), gain_second)
    result = (primal + convolve(second, weight_second)).astype(jnp.bfloat16)
    dresult = (tangent + convolve(dsecond, weight_second)).astype(jnp.bfloat16)
    return (result[None], dresult[None])
```

```python
import functools

import jax
import jax.numpy as jnp
from jax import lax
from jax.experimental import pallas as pl
from jax.experimental.pallas import tpu as pltpu
from jax.sharding import PartitionSpec as P

GROUPS = 32
EPSILON = 1e-05
AXES = ("dp", "height")
BF = jnp.bfloat16
F32 = jnp.float32
STAT_ROWS = 16


def split3(x):
    hi = x.astype(BF)
    rest = x - hi.astype(F32)
    mid = rest.astype(BF)
    low = (rest - mid.astype(F32)).astype(BF)
    return hi, mid, low


def pack_stats(v_sum, t_sum, v_sq, vt):
    rows = jnp.concatenate([v_sum, t_sum, v_sq, vt], axis=0)
    hi, mid, low = split3(rows)
    pad = jnp.zeros((STAT_ROWS - 12, rows.shape[1]), F32)
    return jnp.concatenate([hi.astype(F32), mid.astype(F32), low.astype(F32), pad], axis=0).astype(BF)


def unpack_stats(packed):
    f = packed.astype(F32)
    return f[0:4] + (f[4:8] + f[8:12])


def local_stats(v_rows, t_rows, count):
    v_sum = sum(jnp.sum(v(), axis=0, keepdims=True) for v in v_rows)
    t_sum = sum(jnp.sum(t(), axis=0, keepdims=True) for t in t_rows)
    v_mean = v_sum / count
    t_mean = t_sum / count
    v_sq = 0.0
    vt = 0.0
    for v, t in zip(v_rows, t_rows):
        vc = v() - v_mean
        tc = t() - t_mean
        v_sq = v_sq + jnp.sum(vc * vc, axis=0, keepdims=True)
        vt = vt + jnp.sum(vc * tc, axis=0, keepdims=True)
    return pack_stats(v_sum, t_sum, v_sq, vt)


def group_matrix(chans):
    size = chans // GROUPS
    r = lax.broadcasted_iota(jnp.int32, (chans, 1), 0)
    c = lax.broadcasted_iota(jnp.int32, (1, chans), 1)
    rg = jnp.floor((r.astype(F32) + 0.5) / size)
    cg = jnp.floor((c.astype(F32) + 0.5) / size)
    return jnp.where(rg == cg, 1.0, 0.0).astype(BF)


def group_sum(rows, matrix):
    hi, mid, low = split3(rows)
    dot = functools.partial(jnp.dot, preferred_element_type=F32)
    return dot(hi, matrix) + (dot(mid, matrix) + dot(low, matrix))


def coefficients(stats, gain, count, total):
    chans = gain.shape[1]
    matrix = group_matrix(chans)
    first = stats[0][0:2]
    for s in stats[1:]:
        first = first + s[0:2]
    pad6 = jnp.zeros((6, chans), F32)
    means = group_sum(jnp.concatenate([first, pad6], 0), matrix)[0:2] / total
    mean = means[0:1]
    tmean = means[1:2]
    sq = 0.0
    cross = 0.0
    for s in stats:
        dm = s[0:1] / count - mean
        dt = s[1:2] / count - tmean
        sq = sq + (s[2:3] + count * dm * dm)
        cross = cross + (s[3:4] + count * dm * dt)
    seconds = group_sum(jnp.concatenate([sq, cross, pad6], 0), matrix)[0:2] / total
    inverse = lax.rsqrt(seconds[0:1] + EPSILON)
    scale = gain * inverse
    slope = gain * (seconds[1:2] * (inverse * inverse * inverse))
    return mean, tmean, scale, slope


def activate(v, t, coeff):
    mean, tmean, scale, slope = coeff
    vc = v - mean
    a = vc * scale
    da = (t - tmean) * scale - vc * slope
    s = 0.5 * jnp.tanh(0.5 * a) + 0.5
    h = a * s
    dh = da * (s + h * (1.0 - s))
    return h, dh


def shifted(x):
    cols = x.shape[0]
    idx = lax.broadcasted_iota(jnp.int32, (cols, 1), 0)
    left = jnp.where(idx == 0, 0.0, pltpu.roll(x, 1, 0))
    right = jnp.where(idx == cols - 1, 0.0, pltpu.roll(x, cols - 1, 0))
    return left, right


def edge_buffers(info, first, last, packed, bufx, bufd, bufs):
    cols = first[0].shape[0]
    odd = info[0] == 1
    for k in range(2):
        bufx[k * cols : (k + 1) * cols, :] = jnp.where(odd, first[k], last[k])
        bufd[k * cols : (k + 1) * cols, :] = jnp.where(odd, last[k], first[k])
    bufx[2 * cols :, :] = packed
    bufd[2 * cols :, :] = packed
    bufs[...] = packed


def stats_kernel(info, lat, tan, bufx, bufd, bufs):
    rows, cols, _ = lat.shape
    packed = local_stats(
        [functools.partial(lambda r: lat[r].astype(F32), r) for r in range(rows)],
        [functools.partial(lambda r: tan[r].astype(F32), r) for r in range(rows)],
        float(rows * cols),
    )
    edge_buffers(info, (lat[0], tan[0]), (lat[rows - 1], tan[rows - 1]), packed, bufx, bufd, bufs)


def conv_kernel(final, n_devices, n_pieces, *refs):
    refs = list(refs)
    info = refs.pop(0)
    if final:
        mid_in = refs.pop(0)
        rows, cols = mid_in.shape[0], mid_in.shape[2]
        primal = lambda r: mid_in[r, 0].astype(F32)
        tangent = lambda r: mid_in[r, 1].astype(F32)
        lat, tan = refs.pop(0), refs.pop(0)
    else:
        lat, tan = refs.pop(0), refs.pop(0)
        rows, cols = lat.shape[0], lat.shape[1]
        primal = lambda r: lat[r].astype(F32)
        tangent = lambda r: tan[r].astype(F32)
    xr, dr, yr, own, gain = [refs.pop(0) for _ in range(5)]
    pieces = [refs.pop(0) for _ in range(n_pieces)]
    if final:
        out_p, out_t = refs.pop(0), refs.pop(0)
    else:
        mid_out, bufx, bufd, bufs = [refs.pop(0) for _ in range(4)]
    xs, wv, sems = refs
    chans = gain.shape[1]

    copies = []
    for k, piece in enumerate(pieces):
        height = piece.shape[1]
        offset = pl.multiple_of(info[4 + k], 16)
        for t in range(9):
            copy = pltpu.make_async_copy(
                piece.at[t],
                wv.at[t // 3, pl.ds(offset, height), pl.ds((t % 3) * chans, chans)],
                sems.at[k, t],
            )
            copy.start()
            copies.append(copy)

    count = float(rows * cols)
    total = count * n_devices * (chans // GROUPS)
    stats = [
        unpack_stats(own[...]),
        unpack_stats(xr[2 * cols :, :]),
        unpack_stats(yr[...]),
        unpack_stats(dr[2 * cols :, :]),
    ]
    coeff = coefficients(stats, gain[...], count, total)

    def put(row, h, dh):
        for k, value in enumerate((h, dh)):
            left, right = shifted(value)
            xs[row, k, :, 0:chans] = left.astype(BF)
            xs[row, k, :, chans : 2 * chans] = value.astype(BF)
            xs[row, k, :, 2 * chans : 3 * chans] = right.astype(BF)

    for r in range(rows):
        put(r + 1, *activate(primal(r), tangent(r), coeff))
    odd = info[0] == 1
    xv, xt = xr[0:cols, :].astype(F32), xr[cols : 2 * cols, :].astype(F32)
    dv, dt = dr[0:cols, :].astype(F32), dr[cols : 2 * cols, :].astype(F32)
    for row, flag, v, t in (
        (0, info[1], jnp.where(odd, xv, dv), jnp.where(odd, xt, dt)),
        (rows + 1, info[2], jnp.where(odd, dv, xv), jnp.where(odd, dt, xt)),
    ):
        h, dh = activate(v, t, coeff)
        put(row, jnp.where(flag == 1, h, 0.0), jnp.where(flag == 1, dh, 0.0))

    for copy in copies:
        copy.wait()

    acc = None
    for p in range(3):
        x = xs[p : p + rows].reshape(rows * 2 * cols, 3 * chans)
        term = lax.dot_general(x, wv[p], (((1,), (1,)), ((), ())), preferred_element_type=F32)
        acc = term if acc is None else acc + term
    acc = acc.reshape(rows, 2, cols, chans)
    if final:
        out_p[...] = (lat[...].astype(F32) + acc[:, 0]).astype(BF)
        out_t[...] = (tan[...].astype(F32) + acc[:, 1]).astype(BF)
    else:
        mid_out[...] = acc.astype(BF)
        packed = local_stats(
            [functools.partial(lambda r: mid_out[r, 0].astype(F32), r) for r in range(rows)],
            [functools.partial(lambda r: mid_out[r, 1].astype(F32), r) for r in range(rows)],
            count,
        )
        edge_buffers(
            info, (mid_out[0, 0], mid_out[0, 1]), (mid_out[rows - 1, 0], mid_out[rows - 1, 1]), packed, bufx, bufd, bufs
        )


VM = functools.partial(pl.BlockSpec, memory_space=pltpu.VMEM)
SM = functools.partial(pl.BlockSpec, memory_space=pltpu.SMEM)
HB = functools.partial(pl.BlockSpec, memory_space=pl.ANY)


def fast_device(latents, latent_tangent, gain_first, weight_first, gain_second, weight_second):
    n = lax.axis_size("height")
    nd = lax.axis_size("dp")
    h = lax.axis_index("height")
    core = lax.axis_index("dp") % 2
    rows, cols, chans = latents.shape[1:]
    shard = weight_first.shape[2]

    def permute(x, target):
        pairs = []
        for d in range(nd):
            for i in range(n):
                td, ti = target(d, i)
                pairs.append((d * n + i, td * n + ti))
        return lax.ppermute(x, AXES, pairs)

    def gather(weight, after):
        w = jnp.swapaxes(weight, 1, 2)
        if after is not None:
            w, _ = lax.optimization_barrier((w, after))
        near = permute(w, lambda d, i: (d, i ^ 1) if d % 2 == 0 else (d, i ^ 2))
        half = shard // 2
        fwd = lax.dynamic_slice_in_dim(near, half * (1 - core), half, axis=1)
        diag = permute(fwd, lambda d, i: (d ^ 1, i ^ 2) if d % 2 == 0 else (d ^ 1, i ^ 1))
        near_swap = permute(near, lambda d, i: (d ^ 1, i))
        diag_swap = permute(diag, lambda d, i: (d ^ 1, i))
        return [w, near, near_swap, diag, diag_swap], fwd

    def exchange(bufx, bufd, bufs):
        xr = permute(bufx, lambda d, i: (d, i ^ 1))
        dr = permute(bufd, lambda d, i: (d, i ^ 3))
        yr = permute(bufs, lambda d, i: (d, i ^ 2))
        return xr, dr, yr

    half = shard // 2
    far = shard * (h ^ 3)
    info = jnp.stack(
        [
            h % 2,
            (h > 0).astype(jnp.int32),
            (h < n - 1).astype(jnp.int32),
            core,
            shard * h,
            shard * jnp.where(core == 0, h ^ 1, h ^ 2),
            shard * jnp.where(core == 0, h ^ 2, h ^ 1),
            far + half * core,
            far + half * (1 - core),
        ]
    ).astype(jnp.int32)

    lat = latents[0]
    tan = latent_tangent[0]
    buf = jax.ShapeDtypeStruct((2 * cols + STAT_ROWS, chans), BF)
    small = jax.ShapeDtypeStruct((STAT_ROWS, chans), BF)
    bufx, bufd, own = pl.pallas_call(
        stats_kernel,
        out_shape=(buf, buf, small),
        in_specs=[SM(), VM(), VM()],
        out_specs=(VM(), VM(), VM()),
        name="first_sums",
    )(info, lat, tan)
    got = exchange(bufx, bufd, own)
    first_pieces, sent = gather(weight_first, own)
    second_pieces, _ = gather(weight_second, sent)
    n_pieces = len(first_pieces)
    scratch = [
        pltpu.VMEM((rows + 2, 2, cols, 3 * chans), BF),
        pltpu.VMEM((3, chans, 3 * chans), BF),
        pltpu.SemaphoreType.DMA((n_pieces, 9)),
    ]
    params = pltpu.CompilerParams(vmem_limit_bytes=56 * 1024 * 1024)
    middle, bufx, bufd, own2 = pl.pallas_call(
        functools.partial(conv_kernel, False, n, n_pieces),
        out_shape=(jax.ShapeDtypeStruct((rows, 2, cols, chans), BF), buf, buf, small),
        in_specs=[SM()] + [VM()] * 7 + [HB()] * n_pieces,
        out_specs=(VM(),) * 4,
        scratch_shapes=scratch,
        compiler_params=params,
        name="first_conv",
    )(info, lat, tan, *got, own, gain_first[None], *first_pieces)
    got2 = exchange(bufx, bufd, own2)
    out = jax.ShapeDtypeStruct((rows, cols, chans), BF)
    result, dresult = pl.pallas_call(
        functools.partial(conv_kernel, True, n, n_pieces),
        out_shape=(out, out),
        in_specs=[SM()] + [VM()] * 8 + [HB()] * n_pieces,
        out_specs=(VM(),) * 2,
        scratch_shapes=scratch,
        compiler_params=params,
        name="second_conv",
    )(info, middle, lat, tan, *got2, own2, gain_second[None], *second_pieces)
    return result[None], dresult[None]


def extended(cells, width):
    count = lax.axis_size("height")
    head = lax.slice_in_dim(cells, 0, width, axis=1)
    tail = lax.slice_in_dim(cells, cells.shape[1] - width, cells.shape[1], axis=1)
    up = lax.ppermute(tail, "height", [(i, i + 1) for i in range(count - 1)])
    down = lax.ppermute(head, "height", [(i + 1, i) for i in range(count - 1)])
    return jnp.concatenate([up, cells, down], axis=1)


def plain_normalize(stacked, gain):
    rows, cols, chans = stacked.shape[1:]
    size = chans // GROUPS
    positions = float(rows * cols * size * lax.axis_size("height"))
    grouped = stacked.reshape(2, rows * cols, GROUPS, size)
    mean = lax.psum(jnp.sum(grouped, axis=(1, 3)), "height") / positions
    centered = grouped - mean[:, None, :, None]
    second = lax.psum(jnp.sum(centered * centered[0:1], axis=(1, 3)), "height") / positions
    inverse = lax.rsqrt(second[0] + EPSILON)[None, :, None]
    normed = centered[0] * inverse
    dnormed = centered[1] * inverse - centered[0] * (second[1][None, :, None] * inverse**3)
    a = normed.reshape(rows, cols, chans) * gain
    da = dnormed.reshape(rows, cols, chans) * gain
    s = jax.nn.sigmoid(a)
    return jnp.stack([a * s, da * s * (1.0 + a * (1.0 - s))], 0).astype(BF)


def plain_convolve(hidden, weight):
    rows, cols, chans = hidden.shape[1:]
    padded = jnp.pad(extended(hidden, 1), ((0, 0), (0, 0), (1, 1), (0, 0)))
    full = lax.all_gather(weight, "height", axis=2, tiled=True)
    acc = 0.0
    for t in range(9):
        p, q = t // 3, t % 3
        window = padded[:, p : p + rows, q : q + cols, :].reshape(-1, chans)
        acc = acc + jnp.dot(window, full[t], preferred_element_type=F32)
    return acc.reshape(2, rows, cols, -1)


def plain_device(latents, latent_tangent, gain_first, weight_first, gain_second, weight_second):
    stacked = jnp.concatenate([latents, latent_tangent], 0).astype(F32)
    middle = plain_convolve(plain_normalize(stacked, gain_first), weight_first).astype(BF)
    second = plain_normalize(middle.astype(F32), gain_second)
    result = (stacked + plain_convolve(second, weight_second)).astype(BF)
    return (result[0:1], result[1:2])


def solution(mesh):
    square = mesh.shape["height"] == 4 and mesh.shape["dp"] % 2 == 0
    placed = (
        P("dp", "height", None, None),
        P("dp", "height", None, None),
        P(),
        P(None, None, "height"),
        P(),
        P(None, None, "height"),
    )
    return jax.shard_map(
        fast_device if square else plain_device,
        mesh=mesh,
        in_specs=placed,
        out_specs=(P("dp", "height", None, None), P("dp", "height", None, None)),
        check_vma=False,
    )
```

```python
import functools

import jax
import jax.numpy as jnp
from jax import lax
from jax.experimental import pallas as pl
from jax.experimental.pallas import tpu as pltpu
from jax.sharding import PartitionSpec as P


GROUPS = 32
EPSILON = 1e-05
AXES = ("dp", "height")
BF = jnp.bfloat16
F32 = jnp.float32
STAT_ROWS = 16
VMEM_LIMIT = 32 * 1024 * 1024


def split3(x):
    hi = x.astype(BF)
    rest = x - hi.astype(F32)
    mid = rest.astype(BF)
    low = (rest - mid.astype(F32)).astype(BF)
    return hi, mid, low


def pack_stats(v_sum, t_sum, v_sq, vt):
    rows = jnp.concatenate([v_sum, t_sum, v_sq, vt], axis=0)
    hi, mid, low = split3(rows)
    pad = jnp.zeros((STAT_ROWS - 12, rows.shape[1]), F32)
    return jnp.concatenate([hi.astype(F32), mid.astype(F32), low.astype(F32), pad], axis=0).astype(BF)


def unpack_stats(packed):
    f = packed.astype(F32)
    return f[0:4] + (f[4:8] + f[8:12])


def local_stats(v_rows, t_rows, count):
    v_sum = sum(jnp.sum(v(), axis=0, keepdims=True) for v in v_rows)
    t_sum = sum(jnp.sum(t(), axis=0, keepdims=True) for t in t_rows)
    v_mean = v_sum / count
    t_mean = t_sum / count
    v_sq = 0.0
    vt = 0.0
    for v, t in zip(v_rows, t_rows):
        vc = v() - v_mean
        tc = t() - t_mean
        v_sq = v_sq + jnp.sum(vc * vc, axis=0, keepdims=True)
        vt = vt + jnp.sum(vc * tc, axis=0, keepdims=True)
    return pack_stats(v_sum, t_sum, v_sq, vt)


def group_matrix(chans):
    size = chans // GROUPS
    r = lax.broadcasted_iota(jnp.int32, (chans, 1), 0)
    c = lax.broadcasted_iota(jnp.int32, (1, chans), 1)
    rg = jnp.floor((r.astype(F32) + 0.5) / size)
    cg = jnp.floor((c.astype(F32) + 0.5) / size)
    return jnp.where(rg == cg, 1.0, 0.0).astype(BF)


def group_sum(rows, matrix):
    hi, mid, low = split3(rows)
    dot = functools.partial(jnp.dot, preferred_element_type=F32)
    return dot(hi, matrix) + (dot(mid, matrix) + dot(low, matrix))


def coefficients(stats, gain, count, total):
    chans = gain.shape[1]
    matrix = group_matrix(chans)
    first = stats[0][0:2]
    for s in stats[1:]:
        first = first + s[0:2]
    pad6 = jnp.zeros((6, chans), F32)
    means = group_sum(jnp.concatenate([first, pad6], 0), matrix)[0:2] / total
    mean = means[0:1]
    tmean = means[1:2]
    sq = 0.0
    cross = 0.0
    for s in stats:
        dm = s[0:1] / count - mean
        dt = s[1:2] / count - tmean
        sq = sq + (s[2:3] + count * dm * dm)
        cross = cross + (s[3:4] + count * dm * dt)
    seconds = group_sum(jnp.concatenate([sq, cross, pad6], 0), matrix)[0:2] / total
    inverse = lax.rsqrt(seconds[0:1] + EPSILON)
    scale = gain * inverse
    slope = gain * (seconds[1:2] * (inverse * inverse * inverse))
    return mean, tmean, scale, slope


def activate(v, t, coeff):
    mean, tmean, scale, slope = coeff
    vc = v - mean
    a = vc * scale
    da = (t - tmean) * scale - vc * slope
    s = 0.5 * jnp.tanh(0.5 * a) + 0.5
    h = a * s
    dh = da * (s + h * (1.0 - s))
    return h, dh


def shifted(x):
    cols = x.shape[0]
    idx = lax.broadcasted_iota(jnp.int32, (cols, 1), 0)
    left = jnp.where(idx == 0, 0.0, pltpu.roll(x, 1, 0))
    right = jnp.where(idx == cols - 1, 0.0, pltpu.roll(x, cols - 1, 0))
    return left, right


def send_rows(info, first, last, hx, hd):
    odd = info[ODD] == 1
    for k in range(2):
        hx[k] = jnp.where(odd, first[k], last[k])
        hd[k] = jnp.where(odd, last[k], first[k])


def sums_kernel(info, lat, tan, sums, hx, hd):
    rows, cols, _ = lat.shape
    sums[...] = local_stats(
        [functools.partial(lambda r: lat[r].astype(F32), r) for r in range(rows)],
        [functools.partial(lambda r: tan[r].astype(F32), r) for r in range(rows)],
        float(rows * cols),
    )
    send_rows(info, (lat[0], tan[0]), (lat[rows - 1], tan[rows - 1]), hx, hd)


def put(xs, row, h, dh):
    chans = h.shape[1]
    for k, value in enumerate((h, dh)):
        left, right = shifted(value)
        xs[row, k, :, 0:chans] = left.astype(BF)
        xs[row, k, :, chans : 2 * chans] = value.astype(BF)
        xs[row, k, :, 2 * chans : 3 * chans] = right.astype(BF)


def act_kernel(n_devices, joined, *refs):
    refs = list(refs)
    if joined:
        both = refs.pop(0)
        rows, cols, chans = both.shape[0], both.shape[2], both.shape[3]
        load = lambda r: (both[r, 0].astype(F32), both[r, 1].astype(F32))
    else:
        lat, tan = refs.pop(0), refs.pop(0)
        rows, cols, chans = lat.shape
        load = lambda r: (lat[r].astype(F32), tan[r].astype(F32))
    s0, s1, s2, s3, gain, xs, coeff_out = refs
    count = float(rows * cols)
    total = count * n_devices * (chans // GROUPS)
    coeff = coefficients([unpack_stats(s[...]) for s in (s0, s1, s2, s3)], gain[...], count, total)
    coeff_out[...] = jnp.concatenate(list(coeff) + [jnp.zeros((4, chans), F32)], 0)
    for r in range(rows):
        put(xs, r, *activate(*load(r), coeff))


def fill(wv, piece, tap, offset):
    height, chans = piece.shape[1], piece.shape[2]
    offset = pl.multiple_of(offset, 16)
    for q in range(3):
        wv[pl.ds(offset, height), q * chans : (q + 1) * chans] = piece[tap + q]


def product(x, w):
    return lax.dot_general(x, w, (((1,), (1,)), ((), ())), preferred_element_type=F32)


def rows_product(xs, start, count, wv):
    cols, wide = xs.shape[2], xs.shape[3]
    x = xs[pl.ds(start, count)].reshape(count * 2 * cols, wide)
    return product(x, wv[...]).reshape(count, 2, cols, wv.shape[0])


def main_kernel(info, xs, *refs):
    pieces = refs[:7]
    acc, w0, w2, w1 = refs[7:]
    rows = xs.shape[0]
    for p, wv in ((1, w1), (0, w0), (2, w2)):
        for k, piece in enumerate(pieces):
            fill(wv, piece, 3 * p, info[OFFSETS + k])
        if p == 1:
            acc[...] = rows_product(xs, 0, rows, wv)
        elif p == 0:
            acc[1:rows] = acc[1:rows] + rows_product(xs, 0, rows - 1, wv)
        else:
            acc[0 : rows - 1] = acc[0 : rows - 1] + rows_product(xs, 1, rows - 1, wv)


def edge_kernel(final, info, acc_in, w0, w2, hx, hd, coeff, *refs):
    if final:
        lat, tan, out_p, out_t, halo, acc = refs
    else:
        mid, sums, sx, sd, halo, acc = refs
    rows, cols = acc_in.shape[0], acc_in.shape[2]
    co = tuple(coeff[k : k + 1] for k in range(4))
    odd = info[ODD] == 1
    for slot in range(2):
        pick = odd if slot == 0 else jnp.logical_not(odd)
        flag = info[VALID + slot]
        v = jnp.where(pick, hx[0], hd[0]).astype(F32)
        t = jnp.where(pick, hx[1], hd[1]).astype(F32)
        h, dh = activate(v, t, co)
        put(halo, slot, jnp.where(flag == 1, h, 0.0), jnp.where(flag == 1, dh, 0.0))
    acc[...] = acc_in[...]
    acc[0] = acc[0] + rows_product(halo, 0, 1, w0)[0]
    acc[rows - 1] = acc[rows - 1] + rows_product(halo, 1, 1, w2)[0]
    if final:
        for r in range(rows):
            out_p[r] = (lat[r].astype(F32) + acc[r, 0]).astype(BF)
            out_t[r] = (tan[r].astype(F32) + acc[r, 1]).astype(BF)
    else:
        mid[...] = acc[...].astype(BF)
        sums[...] = local_stats(
            [functools.partial(lambda r: mid[r, 0].astype(F32), r) for r in range(rows)],
            [functools.partial(lambda r: mid[r, 1].astype(F32), r) for r in range(rows)],
            float(rows * cols),
        )
        send_rows(info, (mid[0, 0], mid[0, 1]), (mid[rows - 1, 0], mid[rows - 1, 1]), sx, sd)


VM = functools.partial(pl.BlockSpec, memory_space=pltpu.VMEM)
SM = functools.partial(pl.BlockSpec, memory_space=pltpu.SMEM)
ODD, VALID, OFFSETS = 0, 1, 3


def call(kernel, args, outs, scratch=(), flops=0):
    return pl.pallas_call(
        kernel,
        out_shape=tuple(jax.ShapeDtypeStruct(s, d) for s, d in outs),
        in_specs=[SM() if a.dtype == jnp.int32 else VM() for a in args],
        out_specs=tuple(VM() for _ in outs),
        scratch_shapes=list(scratch),
        compiler_params=pltpu.CompilerParams(vmem_limit_bytes=VMEM_LIMIT),
        cost_estimate=pl.CostEstimate(flops=flops, bytes_accessed=0, transcendentals=0),
    )(*args)


def fast_device(latents, latent_tangent, gain_first, weight_first, gain_second, weight_second):
    n = lax.axis_size("height")
    nd = lax.axis_size("dp")
    h = lax.axis_index("height")
    d = lax.axis_index("dp")
    core = d % 2
    plane = (d // 2) % 2
    rows, cols, chans = latents.shape[1:]
    shard = weight_first.shape[2]
    half = shard // 2

    def permute(x, target, keep=lambda a, i: True):
        pairs = []
        for a in range(nd):
            for i in range(n):
                if keep(a, i):
                    ta, ti = target(a, i)
                    pairs.append((a * n + i, ta * n + ti))
        return lax.ppermute(x, AXES, pairs)

    plane_to = lambda a, i: (a ^ 2, i)
    core_to = lambda a, i: (a ^ 1, i)

    def gather(weight):
        w = jnp.swapaxes(weight, 1, 2)
        role = lambda a: (a % 2) ^ (a // 2 % 2)
        part = lax.dynamic_slice_in_dim(w, half * core, half, axis=1)
        first = permute(part, lambda a, i: (a, i ^ (1 + role(a))))
        relay = permute(first, lambda a, i: (a, i ^ (2 - role(a))))
        plane = permute(first, plane_to)
        first_s = permute(first, core_to)
        relay_s = permute(relay, core_to)
        plane_s = permute(plane, core_to)
        return [w, first, first_s, relay, relay_s, plane, plane_s]

    def exchange(sums, hx, hd):
        xs = permute(sums, lambda a, i: (a, i ^ 1))
        ds = permute(sums, lambda a, i: (a, i ^ 3))
        ys = permute(sums, lambda a, i: (a, i ^ 2))
        xr = permute(hx, lambda a, i: (a, i ^ 1))
        dr = permute(hd, lambda a, i: (a, i ^ 3), lambda a, i: 0 < i < n - 1)
        return (sums, xs, ys, ds), (xr, dr)

    role = core ^ plane
    here, there = half * core, half * (1 - core)
    info = jnp.stack(
        [
            h % 2,
            (h > 0).astype(jnp.int32),
            (h < n - 1).astype(jnp.int32),
            shard * h,
            shard * (h ^ (1 + role)) + here,
            shard * (h ^ (2 - role)) + there,
            shard * (h ^ 3) + here,
            shard * (h ^ 3) + there,
            shard * (h ^ (2 - role)) + here,
            shard * (h ^ (1 + role)) + there,
        ]
    ).astype(jnp.int32)

    lat = latents[0]
    tan = latent_tangent[0]
    edge = ((2, cols, chans), BF)
    small = ((STAT_ROWS, chans), BF)
    wide = ((rows, 2, cols, 3 * chans), BF)
    acc_t = ((rows, 2, cols, chans), F32)
    wrow = ((chans, 3 * chans), BF)
    work = 2 * rows * 2 * cols * 3 * chans * chans

    def block(k, source, gain, sums, hx, hd, pieces, extra, outs):
        stats, edges = exchange(sums, hx, hd)
        xs, coeff = call(
            functools.partial(act_kernel, n, len(source) == 1),
            [*source, *stats, gain[None]],
            [wide, ((8, chans), F32)],
            flops=work // 4,
        )
        acc, w0, w2 = call(main_kernel, [info, xs, *pieces], [acc_t, wrow, wrow], [pltpu.VMEM(*wrow)], flops=2 * work)
        return call(
            functools.partial(edge_kernel, k == 2),
            [info, acc, w0, w2, *edges, coeff, *extra],
            outs,
            [pltpu.VMEM((2, 2, cols, 3 * chans), BF), pltpu.VMEM(*acc_t)],
            flops=work,
        )

    pieces1 = gather(weight_first)
    pieces2 = gather(weight_second)
    sums, hx, hd = call(sums_kernel, [info, lat, tan], [small, edge, edge], flops=work // 4)
    middle, sums, hx, hd = block(
        1, [lat, tan], gain_first, sums, hx, hd, pieces1, [], [((rows, 2, cols, chans), BF), small, edge, edge]
    )
    out = ((rows, cols, chans), BF)
    result, dresult = block(2, [middle], gain_second, sums, hx, hd, pieces2, [lat, tan], [out, out])
    return result[None], dresult[None]


def extended(cells, width):
    count = lax.axis_size("height")
    head = lax.slice_in_dim(cells, 0, width, axis=1)
    tail = lax.slice_in_dim(cells, cells.shape[1] - width, cells.shape[1], axis=1)
    up = lax.ppermute(tail, "height", [(i, i + 1) for i in range(count - 1)])
    down = lax.ppermute(head, "height", [(i + 1, i) for i in range(count - 1)])
    return jnp.concatenate([up, cells, down], axis=1)


def plain_normalize(stacked, gain):
    rows, cols, chans = stacked.shape[1:]
    size = chans // GROUPS
    positions = float(rows * cols * size * lax.axis_size("height"))
    grouped = stacked.reshape(2, rows * cols, GROUPS, size)
    mean = lax.psum(jnp.sum(grouped, axis=(1, 3)), "height") / positions
    centered = grouped - mean[:, None, :, None]
    second = lax.psum(jnp.sum(centered * centered[0:1], axis=(1, 3)), "height") / positions
    inverse = lax.rsqrt(second[0] + EPSILON)[None, :, None]
    normed = centered[0] * inverse
    dnormed = centered[1] * inverse - centered[0] * (second[1][None, :, None] * inverse**3)
    a = normed.reshape(rows, cols, chans) * gain
    da = dnormed.reshape(rows, cols, chans) * gain
    s = jax.nn.sigmoid(a)
    return jnp.stack([a * s, da * s * (1.0 + a * (1.0 - s))], 0).astype(BF)


def plain_convolve(hidden, weight):
    rows, cols, chans = hidden.shape[1:]
    padded = jnp.pad(extended(hidden, 1), ((0, 0), (0, 0), (1, 1), (0, 0)))
    full = lax.all_gather(weight, "height", axis=2, tiled=True)
    acc = 0.0
    for t in range(9):
        p, q = t // 3, t % 3
        window = padded[:, p : p + rows, q : q + cols, :].reshape(-1, chans)
        acc = acc + jnp.dot(window, full[t], preferred_element_type=F32)
    return acc.reshape(2, rows, cols, -1)


def plain_device(latents, latent_tangent, gain_first, weight_first, gain_second, weight_second):
    stacked = jnp.concatenate([latents, latent_tangent], 0).astype(F32)
    middle = plain_convolve(plain_normalize(stacked, gain_first), weight_first).astype(BF)
    second = plain_normalize(middle.astype(F32), gain_second)
    result = (stacked + plain_convolve(second, weight_second)).astype(BF)
    return (result[0:1], result[1:2])


def solution(mesh):
    square = mesh.shape["height"] == 4 and mesh.shape["dp"] % 4 == 0
    placed = (
        P("dp", "height", None, None),
        P("dp", "height", None, None),
        P(),
        P(None, None, "height"),
        P(),
        P(None, None, "height"),
    )
    return jax.shard_map(
        fast_device if square else plain_device,
        mesh=mesh,
        in_specs=placed,
        out_specs=(P("dp", "height", None, None), P("dp", "height", None, None)),
        check_vma=False,
    )
```

```python
import functools

import jax
import jax.numpy as jnp
from jax import lax
from jax.experimental import pallas as pl
from jax.experimental.pallas import tpu as pltpu
from jax.sharding import PartitionSpec as P


GROUPS = 32
EPSILON = 1e-05
AXES = ("dp", "height")
BF = jnp.bfloat16
F32 = jnp.float32
STAT_ROWS = 16
VMEM_LIMIT = 18 * 1024 * 1024


def split3(x):
    hi = x.astype(BF)
    rest = x - hi.astype(F32)
    mid = rest.astype(BF)
    low = (rest - mid.astype(F32)).astype(BF)
    return hi, mid, low


def pack_stats(v_sum, t_sum, v_sq, vt):
    rows = jnp.concatenate([v_sum, t_sum, v_sq, vt], axis=0)
    hi, mid, low = split3(rows)
    pad = jnp.zeros((STAT_ROWS - 12, rows.shape[1]), F32)
    return jnp.concatenate([hi.astype(F32), mid.astype(F32), low.astype(F32), pad], axis=0).astype(BF)


def unpack_stats(packed):
    f = packed.astype(F32)
    return f[0:4] + (f[4:8] + f[8:12])


def local_stats(v_rows, t_rows, count):
    v_sum = sum(jnp.sum(v(), axis=0, keepdims=True) for v in v_rows)
    t_sum = sum(jnp.sum(t(), axis=0, keepdims=True) for t in t_rows)
    v_mean = v_sum / count
    t_mean = t_sum / count
    v_sq = 0.0
    vt = 0.0
    for v, t in zip(v_rows, t_rows):
        vc = v() - v_mean
        tc = t() - t_mean
        v_sq = v_sq + jnp.sum(vc * vc, axis=0, keepdims=True)
        vt = vt + jnp.sum(vc * tc, axis=0, keepdims=True)
    return pack_stats(v_sum, t_sum, v_sq, vt)


def group_matrix(chans):
    size = chans // GROUPS
    r = lax.broadcasted_iota(jnp.int32, (chans, 1), 0)
    c = lax.broadcasted_iota(jnp.int32, (1, chans), 1)
    rg = jnp.floor((r.astype(F32) + 0.5) / size)
    cg = jnp.floor((c.astype(F32) + 0.5) / size)
    return jnp.where(rg == cg, 1.0, 0.0).astype(BF)


def group_sum(rows, matrix):
    parts = jnp.concatenate([p.astype(F32) for p in split3(rows)] + [jnp.zeros_like(rows)], 0).astype(BF)
    sums = jnp.dot(parts, matrix, preferred_element_type=F32)
    return sums[0:8] + (sums[8:16] + sums[16:24])


def coefficients(stats, gain, count, total):
    chans = gain.shape[1]
    matrix = group_matrix(chans)
    first = stats[0][0:2]
    for s in stats[1:]:
        first = first + s[0:2]
    pad6 = jnp.zeros((6, chans), F32)
    means = group_sum(jnp.concatenate([first, pad6], 0), matrix)[0:2] / total
    mean = means[0:1]
    tmean = means[1:2]
    sq = 0.0
    cross = 0.0
    for s in stats:
        dm = s[0:1] / count - mean
        dt = s[1:2] / count - tmean
        sq = sq + (s[2:3] + count * dm * dm)
        cross = cross + (s[3:4] + count * dm * dt)
    seconds = group_sum(jnp.concatenate([sq, cross, pad6], 0), matrix)[0:2] / total
    inverse = lax.rsqrt(seconds[0:1] + EPSILON)
    scale = gain * inverse
    slope = gain * (seconds[1:2] * (inverse * inverse * inverse))
    return mean, tmean, scale, slope


def activate(v, t, coeff):
    mean, tmean, scale, slope = coeff
    vc = v - mean
    a = vc * scale
    da = (t - tmean) * scale - vc * slope
    s = 0.5 * jnp.tanh(0.5 * a) + 0.5
    h = a * s
    dh = da * (s + h * (1.0 - s))
    return h, dh


def shifted(x):
    cols = x.shape[0]
    idx = lax.broadcasted_iota(jnp.int32, (cols, 1), 0)
    left = jnp.where(idx == 0, 0.0, pltpu.roll(x, 1, 0))
    right = jnp.where(idx == cols - 1, 0.0, pltpu.roll(x, cols - 1, 0))
    return left, right


def send_rows(info, first, last, hx, hd):
    odd = info[ODD] == 1
    for k in range(2):
        hx[k] = jnp.where(odd, first[k], last[k])
        hd[k] = jnp.where(odd, last[k], first[k])


def sums_kernel(info, lat, tan, sums, hx, hd):
    rows, cols, _ = lat.shape
    sums[...] = local_stats(
        [functools.partial(lambda r: lat[r].astype(F32), r) for r in range(rows)],
        [functools.partial(lambda r: tan[r].astype(F32), r) for r in range(rows)],
        float(rows * cols),
    )
    send_rows(info, (lat[0], tan[0]), (lat[rows - 1], tan[rows - 1]), hx, hd)


def put(xs, row, h, dh):
    chans = h.shape[1]
    for k, value in enumerate((h, dh)):
        left, right = shifted(value)
        xs[row, k, :, 0:chans] = left.astype(BF)
        xs[row, k, :, chans : 2 * chans] = value.astype(BF)
        xs[row, k, :, 2 * chans : 3 * chans] = right.astype(BF)


def act_kernel(n_devices, joined, *refs):
    refs = list(refs)
    if joined:
        both = refs.pop(0)
        rows, cols, chans = both.shape[0], both.shape[2], both.shape[3]
        load = lambda r: (both[r, 0].astype(F32), both[r, 1].astype(F32))
    else:
        lat, tan = refs.pop(0), refs.pop(0)
        rows, cols, chans = lat.shape
        load = lambda r: (lat[r].astype(F32), tan[r].astype(F32))
    s0, s1, s2, s3, gain, xs, coeff_out = refs
    count = float(rows * cols)
    total = count * n_devices * (chans // GROUPS)
    coeff = coefficients([unpack_stats(s[...]) for s in (s0, s1, s2, s3)], gain[...], count, total)
    coeff_out[...] = jnp.concatenate(list(coeff) + [jnp.zeros((4, chans), F32)], 0)
    for r in range(rows):
        put(xs, r, *activate(*load(r), coeff))


def fill(wv, piece, tap, offset):
    height, chans = piece.shape[1], piece.shape[2]
    offset = pl.multiple_of(offset, 16)
    for q in range(3):
        wv[pl.ds(offset, height), q * chans : (q + 1) * chans] = piece[tap + q]


def product(x, w):
    return lax.dot_general(x, w, (((1,), (1,)), ((), ())), preferred_element_type=F32)


def rows_product(xs, start, count, wv):
    cols, wide = xs.shape[2], xs.shape[3]
    x = xs[pl.ds(start, count)].reshape(count * 2 * cols, wide)
    return product(x, wv[...]).reshape(count, 2, cols, wv.shape[0])


def main_kernel(info, xs, *refs):
    pieces = refs[:7]
    acc, w0, w2, w1 = refs[7:]
    rows = xs.shape[0]
    for p, wv in ((1, w1), (0, w0), (2, w2)):
        for k, piece in enumerate(pieces):
            fill(wv, piece, 3 * p, info[OFFSETS + k])
        if p == 1:
            acc[...] = rows_product(xs, 0, rows, wv)
        elif p == 0:
            acc[1:rows] = acc[1:rows] + rows_product(xs, 0, rows - 1, wv)
        else:
            acc[0 : rows - 1] = acc[0 : rows - 1] + rows_product(xs, 1, rows - 1, wv)


def edge_kernel(final, info, acc_in, w0, w2, hx, hd, coeff, *refs):
    if final:
        lat, tan, out_p, out_t, halo, acc = refs
    else:
        mid, sums, sx, sd, halo, acc = refs
    rows, cols = acc_in.shape[0], acc_in.shape[2]
    co = tuple(coeff[k : k + 1] for k in range(4))
    odd = info[ODD] == 1
    for slot in range(2):
        pick = odd if slot == 0 else jnp.logical_not(odd)
        flag = info[VALID + slot]
        v = jnp.where(pick, hx[0], hd[0]).astype(F32)
        t = jnp.where(pick, hx[1], hd[1]).astype(F32)
        h, dh = activate(v, t, co)
        put(halo, slot, jnp.where(flag == 1, h, 0.0), jnp.where(flag == 1, dh, 0.0))
    acc[...] = acc_in[...]
    acc[0] = acc[0] + rows_product(halo, 0, 1, w0)[0]
    acc[rows - 1] = acc[rows - 1] + rows_product(halo, 1, 1, w2)[0]
    if final:
        for r in range(rows):
            out_p[r] = (lat[r].astype(F32) + acc[r, 0]).astype(BF)
            out_t[r] = (tan[r].astype(F32) + acc[r, 1]).astype(BF)
    else:
        mid[...] = acc[...].astype(BF)
        sums[...] = local_stats(
            [functools.partial(lambda r: mid[r, 0].astype(F32), r) for r in range(rows)],
            [functools.partial(lambda r: mid[r, 1].astype(F32), r) for r in range(rows)],
            float(rows * cols),
        )
        send_rows(info, (mid[0, 0], mid[0, 1]), (mid[rows - 1, 0], mid[rows - 1, 1]), sx, sd)


VM = functools.partial(pl.BlockSpec, memory_space=pltpu.VMEM)
SM = functools.partial(pl.BlockSpec, memory_space=pltpu.SMEM)
ODD, VALID, OFFSETS = 0, 1, 3


def call(kernel, args, outs, scratch=(), flops=0):
    return pl.pallas_call(
        kernel,
        out_shape=tuple(jax.ShapeDtypeStruct(s, d) for s, d in outs),
        in_specs=[SM() if a.dtype == jnp.int32 else VM() for a in args],
        out_specs=tuple(VM() for _ in outs),
        scratch_shapes=list(scratch),
        compiler_params=pltpu.CompilerParams(vmem_limit_bytes=VMEM_LIMIT),
        cost_estimate=pl.CostEstimate(flops=flops, bytes_accessed=0, transcendentals=0),
    )(*args)


def fast_device(latents, latent_tangent, gain_first, weight_first, gain_second, weight_second):
    n = lax.axis_size("height")
    nd = lax.axis_size("dp")
    h = lax.axis_index("height")
    d = lax.axis_index("dp")
    core = d % 2
    plane = (d // 2) % 2
    rows, cols, chans = latents.shape[1:]
    shard = weight_first.shape[2]
    half = shard // 2

    def permute(x, target, keep=lambda a, i: True):
        pairs = []
        for a in range(nd):
            for i in range(n):
                if keep(a, i):
                    ta, ti = target(a, i)
                    pairs.append((a * n + i, ta * n + ti))
        return lax.ppermute(x, AXES, pairs)

    plane_to = lambda a, i: (a ^ 2, i)
    core_to = lambda a, i: (a ^ 1, i)

    def gather(weight):
        w = jnp.swapaxes(weight, 1, 2)
        role = lambda a: (a % 2) ^ (a // 2 % 2)
        part = lax.dynamic_slice_in_dim(w, half * core, half, axis=1)
        first = permute(part, lambda a, i: (a, i ^ (1 + role(a))))
        relay = permute(first, lambda a, i: (a, i ^ (2 - role(a))))
        plane = permute(first, plane_to)
        first_s = permute(first, core_to)
        relay_s = permute(relay, core_to)
        plane_s = permute(plane, core_to)
        return [w, first, first_s, relay, relay_s, plane, plane_s]

    def exchange(sums, hx, hd):
        xs = permute(sums, lambda a, i: (a, i ^ 1))
        ds = permute(sums, lambda a, i: (a, i ^ 3))
        ys = permute(sums, lambda a, i: (a, i ^ 2))
        xr = permute(hx, lambda a, i: (a, i ^ 1))
        dr = permute(hd, lambda a, i: (a, i ^ 3), lambda a, i: 0 < i < n - 1)
        return (sums, xs, ys, ds), (xr, dr)

    role = core ^ plane
    here, there = half * core, half * (1 - core)
    info = jnp.stack(
        [
            h % 2,
            (h > 0).astype(jnp.int32),
            (h < n - 1).astype(jnp.int32),
            shard * h,
            shard * (h ^ (1 + role)) + here,
            shard * (h ^ (2 - role)) + there,
            shard * (h ^ 3) + here,
            shard * (h ^ 3) + there,
            shard * (h ^ (2 - role)) + here,
            shard * (h ^ (1 + role)) + there,
        ]
    ).astype(jnp.int32)

    lat = latents[0]
    tan = latent_tangent[0]
    edge = ((2, cols, chans), BF)
    small = ((STAT_ROWS, chans), BF)
    wide = ((rows, 2, cols, 3 * chans), BF)
    acc_t = ((rows, 2, cols, chans), F32)
    wrow = ((chans, 3 * chans), BF)
    work = 2 * rows * 2 * cols * 3 * chans * chans

    def block(k, source, gain, sums, hx, hd, pieces, extra, outs):
        stats, edges = exchange(sums, hx, hd)
        xs, coeff = call(
            functools.partial(act_kernel, n, len(source) == 1),
            [*source, *stats, gain[None]],
            [wide, ((8, chans), F32)],
            flops=work // 4,
        )
        acc, w0, w2 = call(main_kernel, [info, xs, *pieces], [acc_t, wrow, wrow], [pltpu.VMEM(*wrow)], flops=2 * work)
        return call(
            functools.partial(edge_kernel, k == 2),
            [info, acc, w0, w2, *edges, coeff, *extra],
            outs,
            [pltpu.VMEM((2, 2, cols, 3 * chans), BF), pltpu.VMEM(*acc_t)],
            flops=work,
        )

    pieces1 = gather(weight_first)
    pieces2 = gather(weight_second)
    sums, hx, hd = call(sums_kernel, [info, lat, tan], [small, edge, edge], flops=work // 4)
    middle, sums, hx, hd = block(
        1, [lat, tan], gain_first, sums, hx, hd, pieces1, [], [((rows, 2, cols, chans), BF), small, edge, edge]
    )
    out = ((rows, cols, chans), BF)
    result, dresult = block(2, [middle], gain_second, sums, hx, hd, pieces2, [lat, tan], [out, out])
    return result[None], dresult[None]


def extended(cells, width):
    count = lax.axis_size("height")
    head = lax.slice_in_dim(cells, 0, width, axis=1)
    tail = lax.slice_in_dim(cells, cells.shape[1] - width, cells.shape[1], axis=1)
    up = lax.ppermute(tail, "height", [(i, i + 1) for i in range(count - 1)])
    down = lax.ppermute(head, "height", [(i + 1, i) for i in range(count - 1)])
    return jnp.concatenate([up, cells, down], axis=1)


def plain_normalize(stacked, gain):
    rows, cols, chans = stacked.shape[1:]
    size = chans // GROUPS
    positions = float(rows * cols * size * lax.axis_size("height"))
    grouped = stacked.reshape(2, rows * cols, GROUPS, size)
    mean = lax.psum(jnp.sum(grouped, axis=(1, 3)), "height") / positions
    centered = grouped - mean[:, None, :, None]
    second = lax.psum(jnp.sum(centered * centered[0:1], axis=(1, 3)), "height") / positions
    inverse = lax.rsqrt(second[0] + EPSILON)[None, :, None]
    normed = centered[0] * inverse
    dnormed = centered[1] * inverse - centered[0] * (second[1][None, :, None] * inverse**3)
    a = normed.reshape(rows, cols, chans) * gain
    da = dnormed.reshape(rows, cols, chans) * gain
    s = jax.nn.sigmoid(a)
    return jnp.stack([a * s, da * s * (1.0 + a * (1.0 - s))], 0).astype(BF)


def plain_convolve(hidden, weight):
    rows, cols, chans = hidden.shape[1:]
    padded = jnp.pad(extended(hidden, 1), ((0, 0), (0, 0), (1, 1), (0, 0)))
    full = lax.all_gather(weight, "height", axis=2, tiled=True)
    acc = 0.0
    for t in range(9):
        p, q = t // 3, t % 3
        window = padded[:, p : p + rows, q : q + cols, :].reshape(-1, chans)
        acc = acc + jnp.dot(window, full[t], preferred_element_type=F32)
    return acc.reshape(2, rows, cols, -1)


def plain_device(latents, latent_tangent, gain_first, weight_first, gain_second, weight_second):
    stacked = jnp.concatenate([latents, latent_tangent], 0).astype(F32)
    middle = plain_convolve(plain_normalize(stacked, gain_first), weight_first).astype(BF)
    second = plain_normalize(middle.astype(F32), gain_second)
    result = (stacked + plain_convolve(second, weight_second)).astype(BF)
    return (result[0:1], result[1:2])


def solution(mesh):
    square = mesh.shape["height"] == 4 and mesh.shape["dp"] % 4 == 0
    placed = (
        P("dp", "height", None, None),
        P("dp", "height", None, None),
        P(),
        P(None, None, "height"),
        P(),
        P(None, None, "height"),
    )
    return jax.shard_map(
        fast_device if square else plain_device,
        mesh=mesh,
        in_specs=placed,
        out_specs=(P("dp", "height", None, None), P("dp", "height", None, None)),
        check_vma=False,
    )
```

```python
import functools

import jax
import jax.numpy as jnp
from jax import lax
from jax.experimental import pallas as pl
from jax.experimental.pallas import tpu as pltpu
from jax.sharding import PartitionSpec as P


GROUPS = 32
EPSILON = 1e-05
AXES = ("dp", "height")
BF = jnp.bfloat16
F32 = jnp.float32
STAT_ROWS = 16
VMEM_LIMIT = 18 * 1024 * 1024


def split3(x):
    hi = x.astype(BF)
    rest = x - hi.astype(F32)
    mid = rest.astype(BF)
    low = (rest - mid.astype(F32)).astype(BF)
    return hi, mid, low


def pack_stats(v_sum, t_sum, v_sq, vt):
    rows = jnp.concatenate([v_sum, t_sum, v_sq, vt], axis=0)
    hi, mid, low = split3(rows)
    pad = jnp.zeros((STAT_ROWS - 12, rows.shape[1]), F32)
    return jnp.concatenate([hi.astype(F32), mid.astype(F32), low.astype(F32), pad], axis=0).astype(BF)


def unpack_stats(packed):
    f = packed.astype(F32)
    return f[0:4] + (f[4:8] + f[8:12])


def local_stats(v_rows, t_rows, count):
    v_sum = sum(jnp.sum(v(), axis=0, keepdims=True) for v in v_rows)
    t_sum = sum(jnp.sum(t(), axis=0, keepdims=True) for t in t_rows)
    v_mean = v_sum / count
    t_mean = t_sum / count
    v_sq = 0.0
    vt = 0.0
    for v, t in zip(v_rows, t_rows):
        vc = v() - v_mean
        tc = t() - t_mean
        v_sq = v_sq + jnp.sum(vc * vc, axis=0, keepdims=True)
        vt = vt + jnp.sum(vc * tc, axis=0, keepdims=True)
    return pack_stats(v_sum, t_sum, v_sq, vt)


def group_matrix(chans):
    size = chans // GROUPS
    r = lax.broadcasted_iota(jnp.int32, (chans, 1), 0)
    c = lax.broadcasted_iota(jnp.int32, (1, chans), 1)
    rg = jnp.floor((r.astype(F32) + 0.5) / size)
    cg = jnp.floor((c.astype(F32) + 0.5) / size)
    return jnp.where(rg == cg, 1.0, 0.0).astype(BF)


def group_sum(rows, matrix):
    parts = jnp.concatenate([p.astype(F32) for p in split3(rows)] + [jnp.zeros_like(rows)], 0).astype(BF)
    sums = jnp.dot(parts, matrix, preferred_element_type=F32)
    return sums[0:8] + (sums[8:16] + sums[16:24])


def coefficients(stats, gain, count, total):
    chans = gain.shape[1]
    matrix = group_matrix(chans)
    first = stats[0][0:2]
    for s in stats[1:]:
        first = first + s[0:2]
    pad6 = jnp.zeros((6, chans), F32)
    means = group_sum(jnp.concatenate([first, pad6], 0), matrix)[0:2] / total
    mean = means[0:1]
    tmean = means[1:2]
    sq = 0.0
    cross = 0.0
    for s in stats:
        dm = s[0:1] / count - mean
        dt = s[1:2] / count - tmean
        sq = sq + (s[2:3] + count * dm * dm)
        cross = cross + (s[3:4] + count * dm * dt)
    seconds = group_sum(jnp.concatenate([sq, cross, pad6], 0), matrix)[0:2] / total
    inverse = lax.rsqrt(seconds[0:1] + EPSILON)
    scale = gain * inverse
    slope = gain * (seconds[1:2] * (inverse * inverse * inverse))
    return mean, tmean, scale, slope


def activate(v, t, coeff):
    mean, tmean, scale, slope = coeff
    vc = v - mean
    a = vc * scale
    da = (t - tmean) * scale - vc * slope
    s = 0.5 * jnp.tanh(0.5 * a) + 0.5
    h = a * s
    dh = da * (s + h * (1.0 - s))
    return h, dh


def shifted(x):
    cols = x.shape[0]
    idx = lax.broadcasted_iota(jnp.int32, (cols, 1), 0)
    left = jnp.where(idx == 0, 0.0, pltpu.roll(x, 1, 0))
    right = jnp.where(idx == cols - 1, 0.0, pltpu.roll(x, cols - 1, 0))
    return left, right


def send_rows(info, first, last, hx, hd):
    odd = info[ODD] == 1
    for k in range(2):
        hx[k] = jnp.where(odd, first[k], last[k])
        hd[k] = jnp.where(odd, last[k], first[k])


def sums_kernel(info, lat, tan, sums, hx, hd):
    rows, cols, _ = lat.shape
    sums[...] = local_stats(
        [functools.partial(lambda r: lat[r].astype(F32), r) for r in range(rows)],
        [functools.partial(lambda r: tan[r].astype(F32), r) for r in range(rows)],
        float(rows * cols),
    )
    send_rows(info, (lat[0], tan[0]), (lat[rows - 1], tan[rows - 1]), hx, hd)


def put(xs, row, h, dh):
    chans = h.shape[1]
    for k, value in enumerate((h, dh)):
        left, right = shifted(value)
        xs[row, k, :, 0:chans] = left.astype(BF)
        xs[row, k, :, chans : 2 * chans] = value.astype(BF)
        xs[row, k, :, 2 * chans : 3 * chans] = right.astype(BF)


def act_kernel(n_devices, joined, *refs):
    refs = list(refs)
    if joined:
        both = refs.pop(0)
        rows, cols, chans = both.shape[0], both.shape[2], both.shape[3]
        load = lambda r: (both[r, 0].astype(F32), both[r, 1].astype(F32))
    else:
        lat, tan = refs.pop(0), refs.pop(0)
        rows, cols, chans = lat.shape
        load = lambda r: (lat[r].astype(F32), tan[r].astype(F32))
    s0, s1, s2, s3, gain, xs, coeff_out = refs
    count = float(rows * cols)
    total = count * n_devices * (chans // GROUPS)
    coeff = coefficients([unpack_stats(s[...]) for s in (s0, s1, s2, s3)], gain[...], count, total)
    coeff_out[...] = jnp.concatenate(list(coeff) + [jnp.zeros((4, chans), F32)], 0)
    for r in range(rows):
        put(xs, r, *activate(*load(r), coeff))


def fill(wv, piece, tap, offset):
    height, chans = piece.shape[1], piece.shape[2]
    offset = pl.multiple_of(offset, 16)
    for q in range(3):
        wv[pl.ds(offset, height), q * chans : (q + 1) * chans] = piece[tap + q]


def product(x, w):
    return lax.dot_general(x, w, (((1,), (1,)), ((), ())), preferred_element_type=F32)


def rows_product(xs, start, count, wv):
    cols, wide = xs.shape[2], xs.shape[3]
    x = xs[pl.ds(start, count)].reshape(count * 2 * cols, wide)
    return product(x, wv[...]).reshape(count, 2, cols, wv.shape[0])


def main_kernel(info, xs, *refs):
    pieces = refs[:7]
    acc, w0, w2, w1 = refs[7:]
    rows = xs.shape[0]
    for p, wv in ((1, w1), (0, w0), (2, w2)):
        for k, piece in enumerate(pieces):
            fill(wv, piece, 3 * p, info[OFFSETS + k])
        if p == 1:
            acc[...] = rows_product(xs, 0, rows, wv)
        elif p == 0:
            acc[1:rows] = acc[1:rows] + rows_product(xs, 0, rows - 1, wv)
        else:
            acc[0 : rows - 1] = acc[0 : rows - 1] + rows_product(xs, 1, rows - 1, wv)


def edge_products(info, hx, hd, coeff, w0, w2, halo):
    co = tuple(coeff[k : k + 1] for k in range(4))
    odd = info[ODD] == 1
    for slot in range(2):
        pick = odd if slot == 0 else jnp.logical_not(odd)
        flag = info[VALID + slot]
        v = jnp.where(pick, hx[0], hd[0]).astype(F32)
        t = jnp.where(pick, hx[1], hd[1]).astype(F32)
        h, dh = activate(v, t, co)
        put(halo, slot, jnp.where(flag == 1, h, 0.0), jnp.where(flag == 1, dh, 0.0))
    return rows_product(halo, 0, 1, w0)[0], rows_product(halo, 1, 1, w2)[0]


def first_edge_kernel(info, acc, w0, w2, hx, hd, coeff, mid, sums, sx, sd, halo):
    rows, cols = acc.shape[0], acc.shape[2]
    for r in range(1, rows - 1):
        mid[r] = acc[r].astype(BF)
    head, tail = edge_products(info, hx, hd, coeff, w0, w2, halo)
    mid[0] = (acc[0] + head).astype(BF)
    mid[rows - 1] = (acc[rows - 1] + tail).astype(BF)
    sums[...] = local_stats(
        [functools.partial(lambda r: mid[r, 0].astype(F32), r) for r in range(rows)],
        [functools.partial(lambda r: mid[r, 1].astype(F32), r) for r in range(rows)],
        float(rows * cols),
    )
    send_rows(info, (mid[0, 0], mid[0, 1]), (mid[rows - 1, 0], mid[rows - 1, 1]), sx, sd)


def last_edge_kernel(info, acc, w0, w2, hx, hd, coeff, lat, tan, out_p, out_t, halo, done, sems):
    rows = acc.shape[0]
    copies = []

    def leave(r, value):
        for k, (source, out) in enumerate(((lat, out_p), (tan, out_t))):
            done[k, r] = (source[r].astype(F32) + value[k]).astype(BF)
            copy = pltpu.make_async_copy(done.at[k, r], out.at[r], sems.at[k, r])
            copy.start()
            copies.append(copy)

    for r in range(1, rows - 1):
        leave(r, acc[r])
    head, tail = edge_products(info, hx, hd, coeff, w0, w2, halo)
    leave(0, acc[0] + head)
    leave(rows - 1, acc[rows - 1] + tail)
    for copy in copies:
        copy.wait()


VM = functools.partial(pl.BlockSpec, memory_space=pltpu.VMEM)
SM = functools.partial(pl.BlockSpec, memory_space=pltpu.SMEM)
HB = functools.partial(pl.BlockSpec, memory_space=pl.ANY)
ODD, VALID, OFFSETS = 0, 1, 3


def call(kernel, args, outs, scratch=(), flops=0, place=VM):
    return pl.pallas_call(
        kernel,
        out_shape=tuple(jax.ShapeDtypeStruct(s, d) for s, d in outs),
        in_specs=[SM() if a.dtype == jnp.int32 else VM() for a in args],
        out_specs=tuple(place() for _ in outs),
        scratch_shapes=list(scratch),
        compiler_params=pltpu.CompilerParams(vmem_limit_bytes=VMEM_LIMIT),
        cost_estimate=pl.CostEstimate(flops=flops, bytes_accessed=0, transcendentals=0),
    )(*args)


def fast_device(latents, latent_tangent, gain_first, weight_first, gain_second, weight_second):
    n = lax.axis_size("height")
    nd = lax.axis_size("dp")
    h = lax.axis_index("height")
    d = lax.axis_index("dp")
    core = d % 2
    plane = (d // 2) % 2
    rows, cols, chans = latents.shape[1:]
    shard = weight_first.shape[2]
    half = shard // 2

    def permute(x, target, keep=lambda a, i: True):
        pairs = []
        for a in range(nd):
            for i in range(n):
                if keep(a, i):
                    ta, ti = target(a, i)
                    pairs.append((a * n + i, ta * n + ti))
        return lax.ppermute(x, AXES, pairs)

    plane_to = lambda a, i: (a ^ 2, i)
    core_to = lambda a, i: (a ^ 1, i)

    def gather(weight):
        w = jnp.swapaxes(weight, 1, 2)
        role = lambda a: (a % 2) ^ (a // 2 % 2)
        part = lax.dynamic_slice_in_dim(w, half * core, half, axis=1)
        first = permute(part, lambda a, i: (a, i ^ (1 + role(a))))
        relay = permute(first, lambda a, i: (a, i ^ (2 - role(a))))
        plane = permute(first, plane_to)
        first_s = permute(first, core_to)
        relay_s = permute(relay, core_to)
        plane_s = permute(plane, core_to)
        return [w, first, first_s, relay, relay_s, plane, plane_s]

    def exchange(sums, hx, hd):
        xs = permute(sums, lambda a, i: (a, i ^ 1))
        ds = permute(sums, lambda a, i: (a, i ^ 3))
        ys = permute(sums, lambda a, i: (a, i ^ 2))
        xr = permute(hx, lambda a, i: (a, i ^ 1))
        dr = permute(hd, lambda a, i: (a, i ^ 3))
        return (sums, xs, ys, ds), (xr, dr)

    role = core ^ plane
    here, there = half * core, half * (1 - core)
    info = jnp.stack(
        [
            h % 2,
            (h > 0).astype(jnp.int32),
            (h < n - 1).astype(jnp.int32),
            shard * h,
            shard * (h ^ (1 + role)) + here,
            shard * (h ^ (2 - role)) + there,
            shard * (h ^ 3) + here,
            shard * (h ^ 3) + there,
            shard * (h ^ (2 - role)) + here,
            shard * (h ^ (1 + role)) + there,
        ]
    ).astype(jnp.int32)

    lat = latents[0]
    tan = latent_tangent[0]
    edge = ((2, cols, chans), BF)
    small = ((STAT_ROWS, chans), BF)
    wide = ((rows, 2, cols, 3 * chans), BF)
    acc_t = ((rows, 2, cols, chans), F32)
    wrow = ((chans, 3 * chans), BF)
    work = 2 * rows * 2 * cols * 3 * chans * chans

    def block(k, source, gain, sums, hx, hd, pieces, extra, outs):
        stats, edges = exchange(sums, hx, hd)
        xs, coeff = call(
            functools.partial(act_kernel, n, len(source) == 1),
            [*source, *stats, gain[None]],
            [wide, ((8, chans), F32)],
            flops=work // 4,
        )
        acc, w0, w2 = call(main_kernel, [info, xs, *pieces], [acc_t, wrow, wrow], [pltpu.VMEM(*wrow)], flops=2 * work)
        halo = pltpu.VMEM((2, 2, cols, 3 * chans), BF)
        if k == 2:
            kernel, place = last_edge_kernel, HB
            scratch = [halo, pltpu.VMEM((2, rows, cols, chans), BF), pltpu.SemaphoreType.DMA((2, rows))]
        else:
            kernel, place, scratch = first_edge_kernel, VM, [halo]
        args = [info, acc, w0, w2, *edges, coeff, *extra]
        return call(kernel, args, outs, scratch, work, place)

    pieces1 = gather(weight_first)
    pieces2 = gather(weight_second)
    sums, hx, hd = call(sums_kernel, [info, lat, tan], [small, edge, edge], flops=work // 4)
    middle, sums, hx, hd = block(
        1, [lat, tan], gain_first, sums, hx, hd, pieces1, [], [((rows, 2, cols, chans), BF), small, edge, edge]
    )
    out = ((rows, cols, chans), BF)
    result, dresult = block(2, [middle], gain_second, sums, hx, hd, pieces2, [lat, tan], [out, out])
    return result[None], dresult[None]


def extended(cells, width):
    count = lax.axis_size("height")
    head = lax.slice_in_dim(cells, 0, width, axis=1)
    tail = lax.slice_in_dim(cells, cells.shape[1] - width, cells.shape[1], axis=1)
    up = lax.ppermute(tail, "height", [(i, i + 1) for i in range(count - 1)])
    down = lax.ppermute(head, "height", [(i + 1, i) for i in range(count - 1)])
    return jnp.concatenate([up, cells, down], axis=1)


def plain_normalize(stacked, gain):
    rows, cols, chans = stacked.shape[1:]
    size = chans // GROUPS
    positions = float(rows * cols * size * lax.axis_size("height"))
    grouped = stacked.reshape(2, rows * cols, GROUPS, size)
    mean = lax.psum(jnp.sum(grouped, axis=(1, 3)), "height") / positions
    centered = grouped - mean[:, None, :, None]
    second = lax.psum(jnp.sum(centered * centered[0:1], axis=(1, 3)), "height") / positions
    inverse = lax.rsqrt(second[0] + EPSILON)[None, :, None]
    normed = centered[0] * inverse
    dnormed = centered[1] * inverse - centered[0] * (second[1][None, :, None] * inverse**3)
    a = normed.reshape(rows, cols, chans) * gain
    da = dnormed.reshape(rows, cols, chans) * gain
    s = jax.nn.sigmoid(a)
    return jnp.stack([a * s, da * s * (1.0 + a * (1.0 - s))], 0).astype(BF)


def plain_convolve(hidden, weight):
    rows, cols, chans = hidden.shape[1:]
    padded = jnp.pad(extended(hidden, 1), ((0, 0), (0, 0), (1, 1), (0, 0)))
    full = lax.all_gather(weight, "height", axis=2, tiled=True)
    acc = 0.0
    for t in range(9):
        p, q = t // 3, t % 3
        window = padded[:, p : p + rows, q : q + cols, :].reshape(-1, chans)
        acc = acc + jnp.dot(window, full[t], preferred_element_type=F32)
    return acc.reshape(2, rows, cols, -1)


def plain_device(latents, latent_tangent, gain_first, weight_first, gain_second, weight_second):
    stacked = jnp.concatenate([latents, latent_tangent], 0).astype(F32)
    middle = plain_convolve(plain_normalize(stacked, gain_first), weight_first).astype(BF)
    second = plain_normalize(middle.astype(F32), gain_second)
    result = (stacked + plain_convolve(second, weight_second)).astype(BF)
    return (result[0:1], result[1:2])


def solution(mesh):
    square = mesh.shape["height"] == 4 and mesh.shape["dp"] % 4 == 0
    placed = (
        P("dp", "height", None, None),
        P("dp", "height", None, None),
        P(),
        P(None, None, "height"),
        P(),
        P(None, None, "height"),
    )
    return jax.shard_map(
        fast_device if square else plain_device,
        mesh=mesh,
        in_specs=placed,
        out_specs=(P("dp", "height", None, None), P("dp", "height", None, None)),
        check_vma=False,
    )
```

```python
import functools

import jax
import jax.numpy as jnp
from jax import lax
from jax.experimental import pallas as pl
from jax.experimental.pallas import tpu as pltpu
from jax.sharding import PartitionSpec as P


GROUPS = 32
EPSILON = 1e-05
AXES = ("dp", "height")
BF = jnp.bfloat16
F32 = jnp.float32
STAT_ROWS = 16
VMEM_LIMIT = 18 * 1024 * 1024


def split3(x):
    hi = x.astype(BF)
    rest = x - hi.astype(F32)
    mid = rest.astype(BF)
    low = (rest - mid.astype(F32)).astype(BF)
    return hi, mid, low


def pack_stats(v_sum, t_sum, v_sq, vt):
    rows = jnp.concatenate([v_sum, t_sum, v_sq, vt], axis=0)
    hi, mid, low = split3(rows)
    pad = jnp.zeros((STAT_ROWS - 12, rows.shape[1]), F32)
    return jnp.concatenate([hi.astype(F32), mid.astype(F32), low.astype(F32), pad], axis=0).astype(BF)


def unpack_stats(packed):
    f = packed.astype(F32)
    return f[0:4] + (f[4:8] + f[8:12])


def local_stats(v_rows, t_rows, count):
    v_sum = sum(jnp.sum(v(), axis=0, keepdims=True) for v in v_rows)
    t_sum = sum(jnp.sum(t(), axis=0, keepdims=True) for t in t_rows)
    v_mean = v_sum / count
    t_mean = t_sum / count
    v_sq = 0.0
    vt = 0.0
    for v, t in zip(v_rows, t_rows):
        vc = v() - v_mean
        tc = t() - t_mean
        v_sq = v_sq + jnp.sum(vc * vc, axis=0, keepdims=True)
        vt = vt + jnp.sum(vc * tc, axis=0, keepdims=True)
    return pack_stats(v_sum, t_sum, v_sq, vt)


def group_matrix(chans):
    size = chans // GROUPS
    r = lax.broadcasted_iota(jnp.int32, (chans, 1), 0)
    c = lax.broadcasted_iota(jnp.int32, (1, chans), 1)
    rg = jnp.floor((r.astype(F32) + 0.5) / size)
    cg = jnp.floor((c.astype(F32) + 0.5) / size)
    return jnp.where(rg == cg, 1.0, 0.0).astype(BF)


def group_sum(rows, matrix):
    parts = jnp.concatenate([p.astype(F32) for p in split3(rows)] + [jnp.zeros_like(rows)], 0).astype(BF)
    sums = jnp.dot(parts, matrix, preferred_element_type=F32)
    return sums[0:8] + (sums[8:16] + sums[16:24])


def coefficients(stats, matrix, gain, count, total):
    chans = gain.shape[1]
    first = stats[0][0:2]
    for s in stats[1:]:
        first = first + s[0:2]
    pad6 = jnp.zeros((6, chans), F32)
    means = group_sum(jnp.concatenate([first, pad6], 0), matrix)[0:2] / total
    mean = means[0:1]
    tmean = means[1:2]
    sq = 0.0
    cross = 0.0
    for s in stats:
        dm = s[0:1] / count - mean
        dt = s[1:2] / count - tmean
        sq = sq + (s[2:3] + count * dm * dm)
        cross = cross + (s[3:4] + count * dm * dt)
    seconds = group_sum(jnp.concatenate([sq, cross, pad6], 0), matrix)[0:2] / total
    inverse = lax.rsqrt(seconds[0:1] + EPSILON)
    scale = gain * inverse
    slope = gain * (seconds[1:2] * (inverse * inverse * inverse))
    return mean, tmean, scale, slope


def activate(v, t, coeff):
    mean, tmean, scale, slope = coeff
    vc = v - mean
    a = vc * scale
    da = (t - tmean) * scale - vc * slope
    s = 0.5 * jnp.tanh(0.5 * a) + 0.5
    h = a * s
    dh = da * (s + h * (1.0 - s))
    return h, dh


def shifted(x):
    cols = x.shape[0]
    idx = lax.broadcasted_iota(jnp.int32, (cols, 1), 0)
    left = jnp.where(idx == 0, 0.0, pltpu.roll(x, 1, 0))
    right = jnp.where(idx == cols - 1, 0.0, pltpu.roll(x, cols - 1, 0))
    return left, right


def send_rows(info, first, last, hx, hd):
    odd = info[ODD] == 1
    for k in range(2):
        hx[k] = jnp.where(odd, first[k], last[k])
        hd[k] = jnp.where(odd, last[k], first[k])


def sums_kernel(info, lat, tan, sums, hx, hd, matrix):
    rows, cols, _ = lat.shape
    sums[...] = local_stats(
        [functools.partial(lambda r: lat[r].astype(F32), r) for r in range(rows)],
        [functools.partial(lambda r: tan[r].astype(F32), r) for r in range(rows)],
        float(rows * cols),
    )
    send_rows(info, (lat[0], tan[0]), (lat[rows - 1], tan[rows - 1]), hx, hd)
    matrix[...] = group_matrix(lat.shape[2])


def put(xs, row, h, dh):
    chans = h.shape[1]
    for k, value in enumerate((h, dh)):
        left, right = shifted(value)
        xs[row, k, :, 0:chans] = left.astype(BF)
        xs[row, k, :, chans : 2 * chans] = value.astype(BF)
        xs[row, k, :, 2 * chans : 3 * chans] = right.astype(BF)


def act_kernel(n_devices, joined, *refs):
    refs = list(refs)
    if joined:
        both = refs.pop(0)
        rows, cols, chans = both.shape[0], both.shape[2], both.shape[3]
        load = lambda r: (both[r, 0].astype(F32), both[r, 1].astype(F32))
    else:
        lat, tan = refs.pop(0), refs.pop(0)
        rows, cols, chans = lat.shape
        load = lambda r: (lat[r].astype(F32), tan[r].astype(F32))
    s0, s1, s2, s3, matrix, gain, xs, coeff_out = refs
    count = float(rows * cols)
    total = count * n_devices * (chans // GROUPS)
    coeff = coefficients([unpack_stats(s[...]) for s in (s0, s1, s2, s3)], matrix[...], gain[...], count, total)
    coeff_out[...] = jnp.concatenate(list(coeff) + [jnp.zeros((4, chans), F32)], 0)
    for r in range(rows):
        put(xs, r, *activate(*load(r), coeff))


def fill(wv, piece, tap, offset):
    height, chans = piece.shape[1], piece.shape[2]
    offset = pl.multiple_of(offset, 16)
    for q in range(3):
        wv[pl.ds(offset, height), q * chans : (q + 1) * chans] = piece[tap + q]


def product(x, w):
    return lax.dot_general(x, w, (((1,), (1,)), ((), ())), preferred_element_type=F32)


def rows_product(xs, start, count, wv):
    cols, wide = xs.shape[2], xs.shape[3]
    x = xs[pl.ds(start, count)].reshape(count * 2 * cols, wide)
    return product(x, wv[...]).reshape(count, 2, cols, wv.shape[0])


def main_kernel(info, xs, *refs):
    pieces = refs[:7]
    acc, w0, w2, w1 = refs[7:]
    rows = xs.shape[0]
    for p, wv in ((1, w1), (0, w0), (2, w2)):
        for k, piece in enumerate(pieces):
            fill(wv, piece, 3 * p, info[OFFSETS + k])
        if p == 1:
            acc[...] = rows_product(xs, 0, rows, wv)
        elif p == 0:
            acc[1:rows] = acc[1:rows] + rows_product(xs, 0, rows - 1, wv)
        else:
            acc[0 : rows - 1] = acc[0 : rows - 1] + rows_product(xs, 1, rows - 1, wv)


def edge_products(info, hx, hd, coeff, w0, w2, halo):
    co = tuple(coeff[k : k + 1] for k in range(4))
    odd = info[ODD] == 1
    for slot in range(2):
        pick = odd if slot == 0 else jnp.logical_not(odd)
        flag = info[VALID + slot]
        v = jnp.where(pick, hx[0], hd[0]).astype(F32)
        t = jnp.where(pick, hx[1], hd[1]).astype(F32)
        h, dh = activate(v, t, co)
        put(halo, slot, jnp.where(flag == 1, h, 0.0), jnp.where(flag == 1, dh, 0.0))
    return rows_product(halo, 0, 1, w0)[0], rows_product(halo, 1, 1, w2)[0]


def first_edge_kernel(info, acc, w0, w2, hx, hd, coeff, mid, sums, sx, sd, halo):
    rows, cols = acc.shape[0], acc.shape[2]
    for r in range(1, rows - 1):
        mid[r] = acc[r].astype(BF)
    head, tail = edge_products(info, hx, hd, coeff, w0, w2, halo)
    mid[0] = (acc[0] + head).astype(BF)
    mid[rows - 1] = (acc[rows - 1] + tail).astype(BF)
    sums[...] = local_stats(
        [functools.partial(lambda r: mid[r, 0].astype(F32), r) for r in range(rows)],
        [functools.partial(lambda r: mid[r, 1].astype(F32), r) for r in range(rows)],
        float(rows * cols),
    )
    send_rows(info, (mid[0, 0], mid[0, 1]), (mid[rows - 1, 0], mid[rows - 1, 1]), sx, sd)


def last_edge_kernel(info, acc, w0, w2, hx, hd, coeff, lat, tan, out_p, out_t, halo, done, sems):
    rows = acc.shape[0]
    copies = []

    def leave(r, value):
        for k, (source, out) in enumerate(((lat, out_p), (tan, out_t))):
            done[k, r] = (source[r].astype(F32) + value[k]).astype(BF)
            copy = pltpu.make_async_copy(done.at[k, r], out.at[r], sems.at[k, r])
            copy.start()
            copies.append(copy)

    for r in range(1, rows - 1):
        leave(r, acc[r])
    head, tail = edge_products(info, hx, hd, coeff, w0, w2, halo)
    leave(0, acc[0] + head)
    leave(rows - 1, acc[rows - 1] + tail)
    for copy in copies:
        copy.wait()


VM = functools.partial(pl.BlockSpec, memory_space=pltpu.VMEM)
SM = functools.partial(pl.BlockSpec, memory_space=pltpu.SMEM)
HB = functools.partial(pl.BlockSpec, memory_space=pl.ANY)
ODD, VALID, OFFSETS = 0, 1, 3


def call(kernel, args, outs, scratch=(), flops=0, place=VM):
    return pl.pallas_call(
        kernel,
        out_shape=tuple(jax.ShapeDtypeStruct(s, d) for s, d in outs),
        in_specs=[SM() if a.dtype == jnp.int32 else VM() for a in args],
        out_specs=tuple(place() for _ in outs),
        scratch_shapes=list(scratch),
        compiler_params=pltpu.CompilerParams(vmem_limit_bytes=VMEM_LIMIT),
        cost_estimate=pl.CostEstimate(flops=flops, bytes_accessed=0, transcendentals=0),
    )(*args)


def fast_device(latents, latent_tangent, gain_first, weight_first, gain_second, weight_second):
    n = lax.axis_size("height")
    nd = lax.axis_size("dp")
    h = lax.axis_index("height")
    d = lax.axis_index("dp")
    core = d % 2
    plane = (d // 2) % 2
    rows, cols, chans = latents.shape[1:]
    shard = weight_first.shape[2]
    half = shard // 2

    def permute(x, target, keep=lambda a, i: True):
        pairs = []
        for a in range(nd):
            for i in range(n):
                if keep(a, i):
                    ta, ti = target(a, i)
                    pairs.append((a * n + i, ta * n + ti))
        return lax.ppermute(x, AXES, pairs)

    plane_to = lambda a, i: (a ^ 2, i)
    core_to = lambda a, i: (a ^ 1, i)

    def gather(weight):
        w = jnp.swapaxes(weight, 1, 2)
        role = lambda a: (a % 2) ^ (a // 2 % 2)
        part = lax.dynamic_slice_in_dim(w, half * core, half, axis=1)
        first = permute(part, lambda a, i: (a, i ^ (1 + role(a))))
        relay = permute(first, lambda a, i: (a, i ^ (2 - role(a))))
        plane = permute(first, plane_to)
        first_s = permute(first, core_to)
        relay_s = permute(relay, core_to)
        plane_s = permute(plane, core_to)
        return [w, first, first_s, relay, relay_s, plane, plane_s]

    def exchange(k, sums, hx, hd):
        xs = permute(sums, lambda a, i: (a, i ^ 1))
        ds = permute(sums, lambda a, i: (a, i ^ 3))
        ys = permute(sums, lambda a, i: (a, i ^ 2))
        xr = permute(hx, lambda a, i: (a, i ^ 1))
        dr = permute(hd, lambda a, i: (a, i ^ 3), lambda a, i: k == 2 or 0 < i < n - 1)
        return (sums, xs, ys, ds), (xr, dr)

    role = core ^ plane
    here, there = half * core, half * (1 - core)
    info = jnp.stack(
        [
            h % 2,
            (h > 0).astype(jnp.int32),
            (h < n - 1).astype(jnp.int32),
            shard * h,
            shard * (h ^ (1 + role)) + here,
            shard * (h ^ (2 - role)) + there,
            shard * (h ^ 3) + here,
            shard * (h ^ 3) + there,
            shard * (h ^ (2 - role)) + here,
            shard * (h ^ (1 + role)) + there,
        ]
    ).astype(jnp.int32)

    lat = latents[0]
    tan = latent_tangent[0]
    edge = ((2, cols, chans), BF)
    small = ((STAT_ROWS, chans), BF)
    wide = ((rows, 2, cols, 3 * chans), BF)
    acc_t = ((rows, 2, cols, chans), F32)
    wrow = ((chans, 3 * chans), BF)
    work = 2 * rows * 2 * cols * 3 * chans * chans

    def block(k, source, matrix, gain, sums, hx, hd, pieces, extra, outs):
        stats, edges = exchange(k, sums, hx, hd)
        xs, coeff = call(
            functools.partial(act_kernel, n, len(source) == 1),
            [*source, *stats, matrix, gain[None]],
            [wide, ((8, chans), F32)],
            flops=work // 4,
        )
        acc, w0, w2 = call(main_kernel, [info, xs, *pieces], [acc_t, wrow, wrow], [pltpu.VMEM(*wrow)], flops=2 * work)
        halo = pltpu.VMEM((2, 2, cols, 3 * chans), BF)
        if k == 2:
            kernel, place = last_edge_kernel, HB
            scratch = [halo, pltpu.VMEM((2, rows, cols, chans), BF), pltpu.SemaphoreType.DMA((2, rows))]
        else:
            kernel, place, scratch = first_edge_kernel, VM, [halo]
        args = [info, acc, w0, w2, *edges, coeff, *extra]
        return call(kernel, args, outs, scratch, work, place)

    pieces1 = gather(weight_first)
    pieces2 = gather(weight_second)
    sums, hx, hd, matrix = call(sums_kernel, [info, lat, tan], [small, edge, edge, ((chans, chans), BF)], flops=work // 4)
    middle, sums, hx, hd = block(
        1, [lat, tan], matrix, gain_first, sums, hx, hd, pieces1, [], [((rows, 2, cols, chans), BF), small, edge, edge]
    )
    out = ((rows, cols, chans), BF)
    result, dresult = block(2, [middle], matrix, gain_second, sums, hx, hd, pieces2, [lat, tan], [out, out])
    return result[None], dresult[None]


def extended(cells, width):
    count = lax.axis_size("height")
    head = lax.slice_in_dim(cells, 0, width, axis=1)
    tail = lax.slice_in_dim(cells, cells.shape[1] - width, cells.shape[1], axis=1)
    up = lax.ppermute(tail, "height", [(i, i + 1) for i in range(count - 1)])
    down = lax.ppermute(head, "height", [(i + 1, i) for i in range(count - 1)])
    return jnp.concatenate([up, cells, down], axis=1)


def plain_normalize(stacked, gain):
    rows, cols, chans = stacked.shape[1:]
    size = chans // GROUPS
    positions = float(rows * cols * size * lax.axis_size("height"))
    grouped = stacked.reshape(2, rows * cols, GROUPS, size)
    mean = lax.psum(jnp.sum(grouped, axis=(1, 3)), "height") / positions
    centered = grouped - mean[:, None, :, None]
    second = lax.psum(jnp.sum(centered * centered[0:1], axis=(1, 3)), "height") / positions
    inverse = lax.rsqrt(second[0] + EPSILON)[None, :, None]
    normed = centered[0] * inverse
    dnormed = centered[1] * inverse - centered[0] * (second[1][None, :, None] * inverse**3)
    a = normed.reshape(rows, cols, chans) * gain
    da = dnormed.reshape(rows, cols, chans) * gain
    s = jax.nn.sigmoid(a)
    return jnp.stack([a * s, da * s * (1.0 + a * (1.0 - s))], 0).astype(BF)


def plain_convolve(hidden, weight):
    rows, cols, chans = hidden.shape[1:]
    padded = jnp.pad(extended(hidden, 1), ((0, 0), (0, 0), (1, 1), (0, 0)))
    full = lax.all_gather(weight, "height", axis=2, tiled=True)
    acc = 0.0
    for t in range(9):
        p, q = t // 3, t % 3
        window = padded[:, p : p + rows, q : q + cols, :].reshape(-1, chans)
        acc = acc + jnp.dot(window, full[t], preferred_element_type=F32)
    return acc.reshape(2, rows, cols, -1)


def plain_device(latents, latent_tangent, gain_first, weight_first, gain_second, weight_second):
    stacked = jnp.concatenate([latents, latent_tangent], 0).astype(F32)
    middle = plain_convolve(plain_normalize(stacked, gain_first), weight_first).astype(BF)
    second = plain_normalize(middle.astype(F32), gain_second)
    result = (stacked + plain_convolve(second, weight_second)).astype(BF)
    return (result[0:1], result[1:2])


def solution(mesh):
    square = mesh.shape["height"] == 4 and mesh.shape["dp"] % 4 == 0
    placed = (
        P("dp", "height", None, None),
        P("dp", "height", None, None),
        P(),
        P(None, None, "height"),
        P(),
        P(None, None, "height"),
    )
    return jax.shard_map(
        fast_device if square else plain_device,
        mesh=mesh,
        in_specs=placed,
        out_specs=(P("dp", "height", None, None), P("dp", "height", None, None)),
        check_vma=False,
    )
```

```python
import functools

import jax
import jax.numpy as jnp
from jax import lax
from jax.experimental import pallas as pl
from jax.experimental.pallas import tpu as pltpu
from jax.sharding import PartitionSpec as P


GROUPS = 32
EPSILON = 1e-05
AXES = ("dp", "height")
BF = jnp.bfloat16
F32 = jnp.float32
STAT_ROWS = 16
BLOCK = 256
VMEM_LIMIT = 18 * 1024 * 1024


def split3(x):
    hi = x.astype(BF)
    rest = x - hi.astype(F32)
    mid = rest.astype(BF)
    low = (rest - mid.astype(F32)).astype(BF)
    return hi, mid, low


def pack_stats(v_sum, t_sum, v_sq, vt):
    rows = jnp.concatenate([v_sum, t_sum, v_sq, vt], axis=0)
    hi, mid, low = split3(rows)
    pad = jnp.zeros((STAT_ROWS - 12, rows.shape[1]), F32)
    return jnp.concatenate([hi.astype(F32), mid.astype(F32), low.astype(F32), pad], axis=0).astype(BF)


def unpack_stats(packed):
    f = packed.astype(F32)
    return f[0:4] + (f[4:8] + f[8:12])


def local_stats(v_rows, t_rows, count):
    v_sum = sum(jnp.sum(v(), axis=0, keepdims=True) for v in v_rows)
    t_sum = sum(jnp.sum(t(), axis=0, keepdims=True) for t in t_rows)
    v_mean = v_sum / count
    t_mean = t_sum / count
    v_sq = 0.0
    vt = 0.0
    for v, t in zip(v_rows, t_rows):
        vc = v() - v_mean
        tc = t() - t_mean
        v_sq = v_sq + jnp.sum(vc * vc, axis=0, keepdims=True)
        vt = vt + jnp.sum(vc * tc, axis=0, keepdims=True)
    return pack_stats(v_sum, t_sum, v_sq, vt)


def group_matrix(chans):
    size = chans // GROUPS
    r = lax.broadcasted_iota(jnp.int32, (chans, 1), 0)
    c = lax.broadcasted_iota(jnp.int32, (1, chans), 1)
    rg = jnp.floor((r.astype(F32) + 0.5) / size)
    cg = jnp.floor((c.astype(F32) + 0.5) / size)
    return jnp.where(rg == cg, 1.0, 0.0).astype(BF)


def group_sum(rows, matrix):
    parts = jnp.concatenate([p.astype(F32) for p in split3(rows)] + [jnp.zeros_like(rows)], 0).astype(BF)
    sums = jnp.dot(parts, matrix, preferred_element_type=F32)
    return sums[0:8] + (sums[8:16] + sums[16:24])


def coefficients(stats, matrix, gain, count, total):
    chans = gain.shape[1]
    first = stats[0][0:2]
    for s in stats[1:]:
        first = first + s[0:2]
    pad6 = jnp.zeros((6, chans), F32)
    means = group_sum(jnp.concatenate([first, pad6], 0), matrix)[0:2] / total
    mean = means[0:1]
    tmean = means[1:2]
    sq = 0.0
    cross = 0.0
    for s in stats:
        dm = s[0:1] / count - mean
        dt = s[1:2] / count - tmean
        sq = sq + (s[2:3] + count * dm * dm)
        cross = cross + (s[3:4] + count * dm * dt)
    seconds = group_sum(jnp.concatenate([sq, cross, pad6], 0), matrix)[0:2] / total
    inverse = lax.rsqrt(seconds[0:1] + EPSILON)
    scale = gain * inverse
    slope = gain * (seconds[1:2] * (inverse * inverse * inverse))
    return mean, tmean, scale, slope


def activate(v, t, coeff):
    mean, tmean, scale, slope = coeff
    vc = v - mean
    a = vc * scale
    da = (t - tmean) * scale - vc * slope
    s = 0.5 * jnp.tanh(0.5 * a) + 0.5
    h = a * s
    dh = da * (s + h * (1.0 - s))
    return h, dh


def shifted(x):
    cols = x.shape[0]
    idx = lax.broadcasted_iota(jnp.int32, (cols, 1), 0)
    left = jnp.where(idx == 0, 0.0, pltpu.roll(x, 1, 0))
    right = jnp.where(idx == cols - 1, 0.0, pltpu.roll(x, cols - 1, 0))
    return left, right


def send_rows(info, first, last, hx, hd):
    odd = info[ODD] == 1
    for k in range(2):
        hx[k] = jnp.where(odd, first[k], last[k])
        hd[k] = jnp.where(odd, last[k], first[k])


def sums_kernel(info, lat, tan, sums, hx, hd, matrix):
    rows, cols, _ = lat.shape
    sums[...] = local_stats(
        [functools.partial(lambda r: lat[r].astype(F32), r) for r in range(rows)],
        [functools.partial(lambda r: tan[r].astype(F32), r) for r in range(rows)],
        float(rows * cols),
    )
    send_rows(info, (lat[0], tan[0]), (lat[rows - 1], tan[rows - 1]), hx, hd)
    matrix[...] = group_matrix(lat.shape[2])


def put(xs, row, h, dh):
    chans = h.shape[1]
    for k, value in enumerate((h, dh)):
        left, right = shifted(value)
        xs[row, k, :, 0:chans] = left.astype(BF)
        xs[row, k, :, chans : 2 * chans] = value.astype(BF)
        xs[row, k, :, 2 * chans : 3 * chans] = right.astype(BF)


def act_kernel(n_devices, joined, *refs):
    refs = list(refs)
    if joined:
        both = refs.pop(0)
        rows, cols, chans = both.shape[0], both.shape[2], both.shape[3]
        load = lambda r: (both[r, 0].astype(F32), both[r, 1].astype(F32))
    else:
        lat, tan = refs.pop(0), refs.pop(0)
        rows, cols, chans = lat.shape
        load = lambda r: (lat[r].astype(F32), tan[r].astype(F32))
    s0, s1, s2, s3, matrix, gain, xs, coeff_out = refs
    count = float(rows * cols)
    total = count * n_devices * (chans // GROUPS)
    coeff = coefficients([unpack_stats(s[...]) for s in (s0, s1, s2, s3)], matrix[...], gain[...], count, total)
    coeff_out[...] = jnp.concatenate(list(coeff) + [jnp.zeros((4, chans), F32)], 0)
    for r in range(rows):
        put(xs, r, *activate(*load(r), coeff))


def fill(wv, piece, tap, offset):
    height, chans = piece.shape[1], piece.shape[2]
    offset = pl.multiple_of(offset, 16)
    for q in range(3):
        wv[pl.ds(offset, height), q * chans : (q + 1) * chans] = piece[tap + q]


def product(x, w):
    return lax.dot_general(x, w, (((1,), (1,)), ((), ())), preferred_element_type=F32)


def rows_product(xs, start, count, wv):
    cols, wide = xs.shape[2], xs.shape[3]
    x = xs[pl.ds(start, count)].reshape(count * 2 * cols, wide)
    return product(x, wv[...]).reshape(count, 2, cols, wv.shape[0])


def main_kernel(info, xs, *refs):
    pieces = refs[:7]
    acc, w0, w2, w1, pair = refs[7:]
    rows, chans = xs.shape[0], acc.shape[3]
    block = pair.shape[0]
    full = chans // block * block
    tail = chans - full
    for p, wv in ((1, w1), (0, w0), (2, w2)):
        for k, piece in enumerate(pieces):
            fill(wv, piece, 3 * p, info[OFFSETS + k])
        part = wv.at[0:full]
        if p == 1:
            acc[..., 0:full] = rows_product(xs, 0, rows, part)
            pair[0:tail] = wv[full:chans]
        elif p == 0:
            acc[1:rows, :, :, 0:full] = acc[1:rows, :, :, 0:full] + rows_product(xs, 0, rows - 1, part)
            pair[tail : 2 * tail] = wv[full:chans]
            both = rows_product(xs, 0, rows, pair.at[0 : 2 * tail])
            acc[..., full:chans] = both[..., 0:tail]
            acc[1:rows, :, :, full:chans] = acc[1:rows, :, :, full:chans] + both[0 : rows - 1, :, :, tail : 2 * tail]
        else:
            acc[0 : rows - 1] = acc[0 : rows - 1] + rows_product(xs, 1, rows - 1, wv)


def edge_products(info, hx, hd, coeff, w0, w2, halo):
    co = tuple(coeff[k : k + 1] for k in range(4))
    odd = info[ODD] == 1
    for slot in range(2):
        pick = odd if slot == 0 else jnp.logical_not(odd)
        flag = info[VALID + slot]
        v = jnp.where(pick, hx[0], hd[0]).astype(F32)
        t = jnp.where(pick, hx[1], hd[1]).astype(F32)
        h, dh = activate(v, t, co)
        put(halo, slot, jnp.where(flag == 1, h, 0.0), jnp.where(flag == 1, dh, 0.0))
    return rows_product(halo, 0, 1, w0)[0], rows_product(halo, 1, 1, w2)[0]


def first_edge_kernel(info, acc, w0, w2, hx, hd, coeff, mid, sums, sx, sd, halo):
    rows, cols = acc.shape[0], acc.shape[2]
    for r in range(1, rows - 1):
        mid[r] = acc[r].astype(BF)
    head, tail = edge_products(info, hx, hd, coeff, w0, w2, halo)
    mid[0] = (acc[0] + head).astype(BF)
    mid[rows - 1] = (acc[rows - 1] + tail).astype(BF)
    sums[...] = local_stats(
        [functools.partial(lambda r: mid[r, 0].astype(F32), r) for r in range(rows)],
        [functools.partial(lambda r: mid[r, 1].astype(F32), r) for r in range(rows)],
        float(rows * cols),
    )
    send_rows(info, (mid[0, 0], mid[0, 1]), (mid[rows - 1, 0], mid[rows - 1, 1]), sx, sd)


def last_edge_kernel(info, acc, w0, w2, hx, hd, coeff, lat, tan, out_p, out_t, halo, done, sems):
    rows = acc.shape[0]
    copies = []

    def leave(r, value):
        for k, (source, out) in enumerate(((lat, out_p), (tan, out_t))):
            done[k, r] = (source[r].astype(F32) + value[k]).astype(BF)
            copy = pltpu.make_async_copy(done.at[k, r], out.at[r], sems.at[k, r])
            copy.start()
            copies.append(copy)

    for r in range(1, rows - 1):
        leave(r, acc[r])
    head, tail = edge_products(info, hx, hd, coeff, w0, w2, halo)
    leave(0, acc[0] + head)
    leave(rows - 1, acc[rows - 1] + tail)
    for copy in copies:
        copy.wait()


VM = functools.partial(pl.BlockSpec, memory_space=pltpu.VMEM)
SM = functools.partial(pl.BlockSpec, memory_space=pltpu.SMEM)
HB = functools.partial(pl.BlockSpec, memory_space=pl.ANY)
ODD, VALID, OFFSETS = 0, 1, 3


def call(kernel, args, outs, scratch=(), flops=0, place=VM):
    return pl.pallas_call(
        kernel,
        out_shape=tuple(jax.ShapeDtypeStruct(s, d) for s, d in outs),
        in_specs=[SM() if a.dtype == jnp.int32 else VM() for a in args],
        out_specs=tuple(place() for _ in outs),
        scratch_shapes=list(scratch),
        compiler_params=pltpu.CompilerParams(vmem_limit_bytes=VMEM_LIMIT),
        cost_estimate=pl.CostEstimate(flops=flops, bytes_accessed=0, transcendentals=0),
    )(*args)


def fast_device(latents, latent_tangent, gain_first, weight_first, gain_second, weight_second):
    n = lax.axis_size("height")
    nd = lax.axis_size("dp")
    h = lax.axis_index("height")
    d = lax.axis_index("dp")
    core = d % 2
    plane = (d // 2) % 2
    rows, cols, chans = latents.shape[1:]
    shard = weight_first.shape[2]
    half = shard // 2

    def permute(x, target, keep=lambda a, i: True):
        pairs = []
        for a in range(nd):
            for i in range(n):
                if keep(a, i):
                    ta, ti = target(a, i)
                    pairs.append((a * n + i, ta * n + ti))
        return lax.ppermute(x, AXES, pairs)

    plane_to = lambda a, i: (a ^ 2, i)
    core_to = lambda a, i: (a ^ 1, i)

    def gather(weight):
        w = jnp.swapaxes(weight, 1, 2)
        role = lambda a: (a % 2) ^ (a // 2 % 2)
        part = lax.dynamic_slice_in_dim(w, half * core, half, axis=1)
        first = permute(part, lambda a, i: (a, i ^ (1 + role(a))))
        relay = permute(first, lambda a, i: (a, i ^ (2 - role(a))))
        plane = permute(first, plane_to)
        first_s = permute(first, core_to)
        relay_s = permute(relay, core_to)
        plane_s = permute(plane, core_to)
        return [w, first, first_s, relay, relay_s, plane, plane_s]

    def exchange(k, sums, hx, hd):
        xs = permute(sums, lambda a, i: (a, i ^ 1))
        ds = permute(sums, lambda a, i: (a, i ^ 3))
        ys = permute(sums, lambda a, i: (a, i ^ 2))
        xr = permute(hx, lambda a, i: (a, i ^ 1))
        dr = permute(hd, lambda a, i: (a, i ^ 3), lambda a, i: k == 2 or 0 < i < n - 1)
        return (sums, xs, ys, ds), (xr, dr)

    role = core ^ plane
    here, there = half * core, half * (1 - core)
    info = jnp.stack(
        [
            h % 2,
            (h > 0).astype(jnp.int32),
            (h < n - 1).astype(jnp.int32),
            shard * h,
            shard * (h ^ (1 + role)) + here,
            shard * (h ^ (2 - role)) + there,
            shard * (h ^ 3) + here,
            shard * (h ^ 3) + there,
            shard * (h ^ (2 - role)) + here,
            shard * (h ^ (1 + role)) + there,
        ]
    ).astype(jnp.int32)

    lat = latents[0]
    tan = latent_tangent[0]
    edge = ((2, cols, chans), BF)
    small = ((STAT_ROWS, chans), BF)
    wide = ((rows, 2, cols, 3 * chans), BF)
    acc_t = ((rows, 2, cols, chans), F32)
    wrow = ((chans, 3 * chans), BF)
    work = 2 * rows * 2 * cols * 3 * chans * chans

    def block(k, source, matrix, gain, sums, hx, hd, pieces, extra, outs):
        stats, edges = exchange(k, sums, hx, hd)
        xs, coeff = call(
            functools.partial(act_kernel, n, len(source) == 1),
            [*source, *stats, matrix, gain[None]],
            [wide, ((8, chans), F32)],
            flops=work // 4,
        )
        acc, w0, w2 = call(main_kernel, [info, xs, *pieces], [acc_t, wrow, wrow], [pltpu.VMEM(*wrow), pltpu.VMEM((BLOCK, 3 * chans), BF)], flops=2 * work)
        halo = pltpu.VMEM((2, 2, cols, 3 * chans), BF)
        if k == 2:
            kernel, place = last_edge_kernel, HB
            scratch = [halo, pltpu.VMEM((2, rows, cols, chans), BF), pltpu.SemaphoreType.DMA((2, rows))]
        else:
            kernel, place, scratch = first_edge_kernel, VM, [halo]
        args = [info, acc, w0, w2, *edges, coeff, *extra]
        return call(kernel, args, outs, scratch, work, place)

    pieces1 = gather(weight_first)
    pieces2 = gather(weight_second)
    sums, hx, hd, matrix = call(sums_kernel, [info, lat, tan], [small, edge, edge, ((chans, chans), BF)], flops=work // 4)
    middle, sums, hx, hd = block(
        1, [lat, tan], matrix, gain_first, sums, hx, hd, pieces1, [], [((rows, 2, cols, chans), BF), small, edge, edge]
    )
    out = ((rows, cols, chans), BF)
    result, dresult = block(2, [middle], matrix, gain_second, sums, hx, hd, pieces2, [lat, tan], [out, out])
    return result[None], dresult[None]


def extended(cells, width):
    count = lax.axis_size("height")
    head = lax.slice_in_dim(cells, 0, width, axis=1)
    tail = lax.slice_in_dim(cells, cells.shape[1] - width, cells.shape[1], axis=1)
    up = lax.ppermute(tail, "height", [(i, i + 1) for i in range(count - 1)])
    down = lax.ppermute(head, "height", [(i + 1, i) for i in range(count - 1)])
    return jnp.concatenate([up, cells, down], axis=1)


def plain_normalize(stacked, gain):
    rows, cols, chans = stacked.shape[1:]
    size = chans // GROUPS
    positions = float(rows * cols * size * lax.axis_size("height"))
    grouped = stacked.reshape(2, rows * cols, GROUPS, size)
    mean = lax.psum(jnp.sum(grouped, axis=(1, 3)), "height") / positions
    centered = grouped - mean[:, None, :, None]
    second = lax.psum(jnp.sum(centered * centered[0:1], axis=(1, 3)), "height") / positions
    inverse = lax.rsqrt(second[0] + EPSILON)[None, :, None]
    normed = centered[0] * inverse
    dnormed = centered[1] * inverse - centered[0] * (second[1][None, :, None] * inverse**3)
    a = normed.reshape(rows, cols, chans) * gain
    da = dnormed.reshape(rows, cols, chans) * gain
    s = jax.nn.sigmoid(a)
    return jnp.stack([a * s, da * s * (1.0 + a * (1.0 - s))], 0).astype(BF)


def plain_convolve(hidden, weight):
    rows, cols, chans = hidden.shape[1:]
    padded = jnp.pad(extended(hidden, 1), ((0, 0), (0, 0), (1, 1), (0, 0)))
    full = lax.all_gather(weight, "height", axis=2, tiled=True)
    acc = 0.0
    for t in range(9):
        p, q = t // 3, t % 3
        window = padded[:, p : p + rows, q : q + cols, :].reshape(-1, chans)
        acc = acc + jnp.dot(window, full[t], preferred_element_type=F32)
    return acc.reshape(2, rows, cols, -1)


def plain_device(latents, latent_tangent, gain_first, weight_first, gain_second, weight_second):
    stacked = jnp.concatenate([latents, latent_tangent], 0).astype(F32)
    middle = plain_convolve(plain_normalize(stacked, gain_first), weight_first).astype(BF)
    second = plain_normalize(middle.astype(F32), gain_second)
    result = (stacked + plain_convolve(second, weight_second)).astype(BF)
    return (result[0:1], result[1:2])


def solution(mesh):
    square = mesh.shape["height"] == 4 and mesh.shape["dp"] % 4 == 0
    placed = (
        P("dp", "height", None, None),
        P("dp", "height", None, None),
        P(),
        P(None, None, "height"),
        P(),
        P(None, None, "height"),
    )
    return jax.shard_map(
        fast_device if square else plain_device,
        mesh=mesh,
        in_specs=placed,
        out_specs=(P("dp", "height", None, None), P("dp", "height", None, None)),
        check_vma=False,
    )
```
